32 devices in a mesh: rows: 2 (over core), cols: 4 (over y, x), slabs: 4 (over z).
Axes of the slice: x: 2, y: 2, z: 4, core: 2. Of those that a mesh axis runs over, the one named last changes fastest.
Arguments:
- tracer: float32 [8, 256, 384, 128], P('rows', 'cols', 'slabs'), may hold values from 0.2 to 1.8
- crowding: float32 [8, 256, 384, 128], P('rows', 'cols', 'slabs'), may hold values from 0.5 to 2
Outputs:
- tracer_end: float32 [8, 256, 384, 128], P('rows', 'cols', 'slabs')
The draws below stay inside these ranges and needn't reach their ends.
All inputs are finite; a program needn't handle non-finite values.
Results may differ from the reference program's by a relative error of at most 0.00002.
Values sent between devices are 32-bit elements.
A program may use at most 448 MiB of HBM per device.

```python
import jax
import jax.numpy as jnp
from jax import lax

GRID_Y = 8
GRID_X = 256
GRID_Z = 384
SPECIES = 128
STEPS = 4


def block_levels(key, shape, cuts, smallest, top_value):
    loudness = 1.0
    for dim, shards_of in cuts:
        steps = jax.random.uniform(jax.random.fold_in(jax.random.fold_in(key, 6), dim), (shards_of,), jnp.float32, smallest / len(cuts), top_value / len(cuts))
        loudness = loudness * jnp.repeat(jnp.exp(steps), shape[dim] // shards_of).reshape((-1,) + (1,) * (len(shape) - 1 - dim))
    return loudness


def setup_inputs(seed: int = 0) -> dict:
    key_of = jax.random.split(jax.random.key(seed), 3)
    return {
        "tracer": jnp.clip(0.2 + 1.5999999 * jax.random.uniform(key_of[0], (GRID_Y, GRID_X, GRID_Z, SPECIES), jnp.float32) ** block_levels(key_of[0], (GRID_Y, GRID_X, GRID_Z, SPECIES), ((0, 2), (1, 4), (2, 4)), -0.2, 0.2), 0.2, 1.8),
        "crowding": jnp.clip(0.5 + 1.5 * jax.random.uniform(key_of[1], (GRID_Y, GRID_X, GRID_Z, SPECIES), jnp.float32) ** block_levels(key_of[1], (GRID_Y, GRID_X, GRID_Z, SPECIES), ((0, 2), (1, 4), (2, 4)), -0.2, 0.2), 0.5, 2.0),
    }


def inner_cells(values, dims):
    for dim in dims:
        values = lax.slice_in_dim(values, 1, values.shape[dim] - 1, axis=dim)
    return values


def side_cells(values, dim, start, dims):
    others = [other for other in dims if other != dim]
    values = inner_cells(values, others)
    return lax.slice_in_dim(values, start, start + values.shape[dim] - 2, axis=dim)


def advance(padded, crowding):
    middle = inner_cells(padded, (0, 1, 2))
    lower = [side_cells(padded, dim, 0, (0, 1, 2)) for dim in (0, 1, 2)]
    upper = [side_cells(padded, dim, 2, (0, 1, 2)) for dim in (0, 1, 2)]
    spread = lower[0] + upper[0] + lower[1] + upper[1] + lower[2] + upper[2] - 6.0 * middle
    return middle + 0.1 * spread + 0.2 * middle * (1.0 - middle * crowding)


def reference(tracer, crowding):
    for step in range(STEPS):
        tracer = advance(jnp.pad(tracer, ((1, 1), (1, 1), (1, 1), (0, 0)), mode="constant"), crowding)
    return tracer
```

```python
import functools

import jax
import jax.numpy as jnp
from jax import lax
from jax.experimental import pallas as pl
from jax.experimental.pallas import tpu as pltpu
from jax.sharding import PartitionSpec as P

STEPS = 4
EDGE = 2
VIA = {1: 3, 2: 0}
LATE = 2
FIRST = 0
PAD = 8
VMEM_LIMIT = 40 * 1024 * 1024
MESH = pl.DeviceIdType.MESH
AXES = ("rows", "cols", "slabs")


def write(ended, out, store_sem):
    rows, width, depth, species = out.shape
    copies = [pltpu.make_async_copy(
        ended.at[1 + y, pl.ds(1, width), pl.ds(PAD, depth)], out.at[y], store_sem.at[y])
        for y in range(rows)]
    for copy in copies:
        copy.start()
    for copy in copies:
        copy.wait()


def kernel(sizes, via, tracer, crowding, ended, other_field, limit, load_sem,
           y_send, y_recv, z_send, z_recv, e_send, e_recv, x_send, x_recv,
           relayed, r_recv, f_send):
    rows, width, depth, species = tracer.shape
    slots = rows
    middle = (width - 2 * EDGE) // slots
    last = slots + 1
    half = rows // 2 if rows % 2 == 0 else rows
    share = rows // 2
    field = (ended, other_field)
    place = {axis: lax.axis_index(axis) for axis in AXES}
    has = {(axis, side): (place[axis] > 0) if side == 0 else (place[axis] < sizes[axis] - 1)
           for axis in AXES for side in (0, 1)}
    near = {(axis, side): {axis: jnp.clip(place[axis] + 2 * side - 1, 0, sizes[axis] - 1)}
            for axis in AXES for side in (0, 1)}
    col = place["cols"]
    upward = lax.rem(place["rows"], 2) == 1
    inner = pl.ds(PAD, depth)

    def row(j):
        return jnp.where(upward, j, rows - 1 - j)

    def span(k):
        if isinstance(k, int):
            if k == 0:
                return 0, EDGE
            if k == last:
                return width - EDGE, EDGE
        return EDGE + (k - 1) * middle, middle

    def remote(axis, to, src, dst, send, recv):
        return pltpu.make_async_remote_copy(
            src_ref=src, dst_ref=dst, send_sem=send, recv_sem=recv,
            device_id=near[axis, to], device_id_type=MESH)

    def y_face(side, p, k, from_input, to):
        start, count = span(k)
        cells, other = pl.ds(1 + start, count), 1 - side
        src = (tracer.at[side * (rows - 1), pl.ds(start, count)] if from_input
               else field[p].at[1 + side * (rows - 1), cells, inner])
        return remote("rows", to, src, field[p].at[other * (rows + 1), cells, inner],
                      y_send.at[p, side, k], y_recv.at[p, other, k])

    def z_face(side, p, k, from_input, to):
        start, count = span(k)
        cells, other, ys = pl.ds(1 + start, count), 1 - side, pl.ds(1, rows)
        src = (tracer.at[:, pl.ds(start, count), pl.ds(side * (depth - 1), 1)] if from_input
               else field[p].at[ys, cells, pl.ds(PAD + side * (depth - 1), 1)])
        return remote("slabs", to, src, field[p].at[ys, cells, pl.ds(PAD - 1 + other * (depth + 1), 1)],
                      z_send.at[p, side, k], z_recv.at[p, other, k])

    def e_face(side, p, edge, group, from_input, to):
        start, count = span(edge * last)
        cells, other = pl.ds(1 + start, count), 1 - side
        first = jnp.where(upward, group * half, rows - (group + 1) * half)
        src = (tracer.at[pl.ds(first, half), pl.ds(start, count), pl.ds(side * (depth - 1), 1)] if from_input
               else field[p].at[pl.ds(1 + first, half), cells, pl.ds(PAD + side * (depth - 1), 1)])
        dst = field[p].at[pl.ds(1 + first, half), cells, pl.ds(PAD - 1 + other * (depth + 1), 1)]
        return remote("slabs", to, src, dst, e_send.at[p, side, edge, group], e_recv.at[p, other, edge, group])

    def x_source(side, event, j, from_input):
        return (tracer.at[row(j), side * (width - 1)] if from_input
                else field[event % 2].at[1 + row(j), 1 + side * (width - 1), inner])

    def x_face(side, event, j, from_input, to):
        p, other = event % 2, 1 - side
        return remote("cols", to, x_source(side, event, j, from_input),
                      field[p].at[1 + row(j), other * (width + 1), inner],
                      x_send.at[p, side, j], x_recv.at[p, other, j])

    def first_relayed(event):
        return 0 if event % 2 == 0 else rows - share

    def first_hop(source, event, j, from_input):
        side, n = 2 - source, j - first_relayed(event)
        return pltpu.make_async_remote_copy(
            src_ref=x_source(side, event, j, from_input), dst_ref=relayed.at[event, n],
            send_sem=x_send.at[event % 2, side, j], recv_sem=r_recv.at[event, n],
            device_id={"cols": via[source]}, device_id_type=MESH)

    def second_hop(source, event, j):
        side, n, p = 2 - source, j - first_relayed(event), event % 2
        return pltpu.make_async_remote_copy(
            src_ref=relayed.at[event, n],
            dst_ref=field[p].at[1 + row(j), (1 - side) * (width + 1), inner],
            send_sem=f_send.at[event, n], recv_sem=x_recv.at[p, 1 - side, j],
            device_id={"cols": 3 - source}, device_id_type=MESH)

    def send_x(side, event, j, from_input=False):
        if not via:
            pl.when(has["cols", side])(lambda: x_face(side, event, j, from_input, side).start())
            return
        first = first_relayed(event)
        relay = jnp.logical_and(col == 2 - side, jnp.logical_and(j >= first, j < first + share))
        pl.when(relay)(lambda: first_hop(2 - side, event, j, from_input).start())
        pl.when(jnp.logical_and(has["cols", side], jnp.logical_not(relay)))(
            lambda: x_face(side, event, j, from_input, side).start())

    def forward(event, j):
        for source in (1, 2):
            @pl.when(col == via[source])
            def _():
                n = j - first_relayed(event)
                pltpu.make_async_remote_copy(
                    src_ref=relayed.at[event, n], dst_ref=relayed.at[event, n],
                    send_sem=f_send.at[event, n], recv_sem=r_recv.at[event, n],
                    device_id={"cols": 3 - source}, device_id_type=MESH).wait_recv()
                second_hop(source, event, j).start()

    def by_side(axis, action):
        for side in (0, 1):
            pl.when(has[axis, side])(functools.partial(action, side))

    tracer_parts = [(0, EDGE + 1)]
    tracer_parts += [(EDGE + k * middle + 1, middle) for k in range(slots - 1)]
    tracer_parts += [(EDGE + (slots - 1) * middle + 1, middle - 2), (width - EDGE - 1, EDGE + 1)]

    def load_tracer(k):
        start, count = tracer_parts[k]
        return pltpu.make_async_copy(
            tracer.at[:, pl.ds(start, count)],
            field[0].at[pl.ds(1, rows), pl.ds(1 + start, count), inner], load_sem.at[0, k])

    def load_limit(k):
        start, count = span(k)
        return pltpu.make_async_copy(
            crowding.at[:, pl.ds(start, count)], limit.at[:, pl.ds(start, count)], load_sem.at[1, k])

    barrier = pltpu.get_barrier_semaphore()
    for axis in AXES:
        by_side(axis, lambda side: pl.semaphore_signal(
            barrier, inc=1, device_id=near[axis, side], device_id_type=MESH))
    if via:
        pl.semaphore_signal(barrier, inc=1, device_id={"cols": lax.rem(col + 2, 4)}, device_id_type=MESH)
    for k in (0, last, 1):
        load_tracer(k).start()
    for k in (1, 0, last):
        load_limit(k).start()
    for k in range(2, last):
        load_tracer(k).start()
        load_limit(k).start()
    pl.semaphore_wait(barrier, (1 if via else 0) + sum(jnp.where(has[key], 1, 0) for key in has))

    for j in range(rows):
        for side in (0, 1):
            send_x(side, 0, j, True)
    for k in [1, 0, last, *range(2, last)]:
        by_side("rows", lambda side: y_face(side, 0, k, True, side).start())
        if k in (0, last):
            for group in range(rows // half):
                by_side("slabs", lambda side: e_face(side, 0, k // last, group, True, side).start())
        else:
            by_side("slabs", lambda side: z_face(side, 0, k, True, side).start())

    def clear(axis, side):
        @pl.when(jnp.logical_not(has[axis, side]))
        def _():
            for p in (0, 1):
                if axis == "rows":
                    @pl.loop(1, width + 1)
                    def _(x):
                        field[p][side * (rows + 1), x, inner] = jnp.zeros((depth, species), jnp.float32)
                elif axis == "cols":
                    @pl.loop(1, rows + 1)
                    def _(y):
                        field[p][y, side * (width + 1), inner] = jnp.zeros((depth, species), jnp.float32)
                else:
                    @pl.loop(1, width + 1)
                    def _(x):
                        for y in range(1, rows + 1):
                            field[p][y, x, pl.ds(PAD - 1 + side * (depth + 1), 1)] = jnp.zeros((1, species), jnp.float32)

    for axis in AXES:
        for side in (0, 1):
            clear(axis, side)

    def scale(step):
        return 0.2 if step == 0 else 0.05 if step == STEPS - 1 else 0.1

    def advance(step, k):
        p = step % 2
        start, count = span(k)

        @pl.loop(0, depth // 8)
        def _(tile):
            at = pl.multiple_of(PAD + tile * 8, 8)
            source = pl.multiple_of(tile * 8, 8)

            def cell(y, x, shift=0):
                return field[p][y, 1 + start + x, pl.ds(at + shift, 8)]

            before = [cell(y, -1) for y in range(1, rows + 1)]
            here = [cell(y, 0) for y in range(1, rows + 1)]
            for x in range(count):
                after = [cell(y, x + 1) for y in range(1, rows + 1)]
                column = [cell(0, x), *here, cell(rows + 1, x)]
                for y in range(rows):
                    here_y = here[y]
                    around = (before[y] + after[y]) + (column[y] + column[y + 2])
                    around = around + (cell(y + 1, x, -1) + cell(y + 1, x, 1))
                    bound = limit[y, start + x, pl.ds(source, 8)]
                    if step == 0:
                        bound = bound + bound
                    field[1 - p][y + 1, 1 + start + x, pl.ds(at, 8)] = scale(step) * (
                        around + here_y * (6.0 - bound * here_y))
                before, here = here, after

    def advance_edges(step, y):
        p = step % 2
        tiles = depth // 8
        group = next(g for g in (4, 3, 2, 1) if tiles % g == 0)

        @pl.loop(0, tiles // group)
        def _(block):
            for n in range(group):
                at = pl.multiple_of(PAD + block * (8 * group) + 8 * n, 8)
                source = pl.multiple_of(block * (8 * group) + 8 * n, 8)
                for edge in (0, 1):
                    start = edge * (width - EDGE)

                    def cell(x, shift=0, up=0):
                        return field[p][1 + y + up, 1 + start + x, pl.ds(at + shift, 8)]

                    line = [cell(x) for x in range(-1, EDGE + 1)]
                    for x in range(EDGE):
                        here = line[x + 1]
                        around = (line[x] + line[x + 2]) + (cell(x, 0, -1) + cell(x, 0, 1))
                        around = around + (cell(x, -1) + cell(x, 1))
                        bound = limit[y, start + x, pl.ds(source, 8)]
                        if step == 0:
                            bound = bound + bound
                        field[1 - p][1 + y, 1 + start + x, pl.ds(at, 8)] = scale(step) * (
                            around + here * (6.0 - bound * here))

    def centre(step, k):
        p = step % 2
        if step == 0:
            load_limit(k).wait()
        by_side("rows", lambda side: y_face(1 - side, p, k, False, side).wait_recv())
        by_side("slabs", lambda side: z_face(1 - side, p, k, False, side).wait_recv())
        if step >= 1:
            by_side("rows", lambda side: y_face(side, 1 - p, k, False, side).wait_send())
            by_side("slabs", lambda side: z_face(side, 1 - p, k, False, side).wait_send())
        advance(step, k)
        if step < STEPS - 1:
            by_side("rows", lambda side: y_face(side, 1 - p, k, False, side).start())
            by_side("slabs", lambda side: z_face(side, 1 - p, k, False, side).start())

    def edges(step, j):
        p = step % 2
        y = row(j)
        group = j // half

        def at_row(side):
            return jnp.logical_and(has["rows", side], y == side * (rows - 1))

        for side in (0, 1):
            @pl.when(at_row(side))
            def _():
                for k in (0, last):
                    y_face(1 - side, p, k, False, side).wait_recv()
                    if step >= 1:
                        y_face(side, 1 - p, k, False, side).wait_send()

        @pl.when(lax.rem(j, half) == 0)
        def _():
            for edge in (0, 1):
                by_side("slabs", lambda side: e_face(1 - side, p, edge, group, False, side).wait_recv())
                if step >= 1:
                    by_side("slabs", lambda side: e_face(side, 1 - p, edge, group, False, side).wait_send())

        by_side("cols", lambda side: x_face(1 - side, step, j, False, side).wait_recv())
        if step >= 1:
            by_side("cols", lambda side: x_face(side, step - 1, j, False, side).wait_send())
        advance_edges(step, y)
        if step < STEPS - 1:
            for side in (0, 1):
                send_x(side, step + 1, j)
            for side in (0, 1):
                @pl.when(at_row(side))
                def _():
                    for k in (0, last):
                        y_face(side, 1 - p, k, False, side).start()

            @pl.when(lax.rem(j, half) == half - 1)
            def _():
                for edge in (0, 1):
                    by_side("slabs", lambda side: e_face(side, 1 - p, edge, group, False, side).start())

    forwards = {}
    if via:
        for event in range(STEPS):
            for n in range(share):
                j = first_relayed(event) + n
                when = (FIRST + n) if event == 0 else (event - 1) * slots + j + LATE
                forwards.setdefault(min(when, STEPS * slots - 1), []).append((event, j))

    for step in range(STEPS):
        if step == 0:
            for k in (0, last, 1):
                load_tracer(k).wait()

        @pl.loop(0, slots)
        def _(slot):
            if step == 0:
                for k in range(2, last):
                    pl.when(slot == k - 1)(functools.partial(lambda k: load_tracer(k).wait(), k))
                centre(step, slot + 1)

                @pl.when(slot == 0)
                def _():
                    for k in (0, last):
                        load_limit(k).wait()
            edges(step, slot)
            for n in range(slots):
                for event, j in forwards.get(step * slots + n, []):
                    pl.when(slot == n)(functools.partial(forward, event, j))
            if step > 0:
                centre(step, slot + 1)

    p = (STEPS - 1) % 2

    @pl.loop(1, last)
    def _(k):
        by_side("rows", lambda side: y_face(side, p, k, False, side).wait_send())
        by_side("slabs", lambda side: z_face(side, p, k, False, side).wait_send())

    for k in (0, last):
        by_side("rows", lambda side: y_face(side, p, k, False, side).wait_send())
        for group in range(rows // half):
            by_side("slabs", lambda side: e_face(side, p, k // last, group, False, side).wait_send())
    for j in range(rows):
        by_side("cols", lambda side: x_face(side, STEPS - 1, j, False, side).wait_send())
    for when in sorted(forwards):
        for event, j in forwards[when]:
            for source in (1, 2):
                pl.when(col == via[source])(lambda: second_hop(source, event, j).wait_send())


def relays(mesh):
    if mesh.shape["cols"] != 4:
        return None
    devices = mesh.devices.transpose([mesh.axis_names.index(axis) for axis in AXES])[0, :, 0]
    chips = [getattr(device, "coords", None) for device in devices]
    if any(chip is None for chip in chips):
        return None
    apart = sum(a != b for a, b in zip(chips[1], chips[2]))
    return VIA if apart > 1 else None


def solution(mesh):
    sizes = dict(mesh.shape)
    via = relays(mesh)

    def on_device(tracer, crowding):
        rows, width, depth, species = tracer.shape
        half = rows // 2 if rows % 2 == 0 else rows
        groups, share, parts = rows // half, max(1, rows // 2), rows + 2
        dma = pltpu.SemaphoreType.DMA
        padded = (rows + 2, width + 2, depth + 2 * PAD, species)
        cell_count = rows * width * depth * species
        ended = pl.pallas_call(
            functools.partial(kernel, sizes, via),
            out_shape=pltpu.VMEM(padded, jnp.float32),
            in_specs=[pl.BlockSpec(memory_space=pl.ANY)] * 2,
            out_specs=pl.BlockSpec(memory_space=pltpu.VMEM),
            scratch_shapes=[
                pltpu.VMEM(padded, jnp.float32),
                pltpu.VMEM(tracer.shape, jnp.float32),
                dma((2, parts)),
                dma((2, 2, parts)), dma((2, 2, parts)),
                dma((2, 2, parts)), dma((2, 2, parts)),
                dma((2, 2, 2, groups)), dma((2, 2, 2, groups)),
                dma((2, 2, rows)), dma((2, 2, rows)),
                pltpu.VMEM((STEPS, share, depth, species), jnp.float32),
                dma((STEPS, share)), dma((STEPS, share)),
            ],
            compiler_params=pltpu.CompilerParams(
                collective_id=0, has_side_effects=True, vmem_limit_bytes=VMEM_LIMIT),
        )(tracer, crowding)
        return pl.pallas_call(
            write,
            out_shape=jax.ShapeDtypeStruct(tracer.shape, jnp.float32),
            in_specs=[pl.BlockSpec(memory_space=pltpu.VMEM)],
            out_specs=pl.BlockSpec(memory_space=pl.ANY),
            scratch_shapes=[dma((rows,))],
            compiler_params=pltpu.CompilerParams(vmem_limit_bytes=1 << 20),
        )(ended)

    return jax.shard_map(
        on_device, mesh=mesh,
        in_specs=(P("rows", "cols", "slabs", None), P("rows", "cols", "slabs", None)),
        out_specs=P("rows", "cols", "slabs", None), check_vma=False)
```

```python
import functools

import jax
import jax.numpy as jnp
from jax import lax
from jax.experimental import pallas as pl
from jax.experimental.pallas import tpu as pltpu
from jax.sharding import PartitionSpec as P

STEPS = 4
EDGE = 2
VIA = {1: 3, 2: 0}
LATE = 2
FIRST = 0
PAD = 8
VMEM_LIMIT = 40 * 1024 * 1024
MESH = pl.DeviceIdType.MESH
AXES = ("rows", "cols", "slabs")


def write(ended, out, store_sem):
    rows, width, depth, species = out.shape
    copies = [pltpu.make_async_copy(
        ended.at[1 + y, pl.ds(1, width), pl.ds(PAD, depth)], out.at[y], store_sem.at[y])
        for y in range(rows)]
    for copy in copies:
        copy.start()
    for copy in copies:
        copy.wait()


def kernel(sizes, via, tracer, crowding, ended, other_field, limit, load_sem,
           y_send, y_recv, z_send, z_recv, e_send, e_recv, x_send, x_recv,
           relayed, r_recv, f_send):
    rows, width, depth, species = tracer.shape
    slots = rows
    middle = (width - 2 * EDGE) // slots
    last = slots + 1
    half = rows // 2 if rows % 2 == 0 else rows
    share = rows // 2
    field = (ended, other_field)
    place = {axis: lax.axis_index(axis) for axis in AXES}
    has = {(axis, side): (place[axis] > 0) if side == 0 else (place[axis] < sizes[axis] - 1)
           for axis in AXES for side in (0, 1)}
    near = {(axis, side): {axis: jnp.clip(place[axis] + 2 * side - 1, 0, sizes[axis] - 1)}
            for axis in AXES for side in (0, 1)}
    col = place["cols"]
    upward = lax.rem(place["rows"], 2) == 1
    inner = pl.ds(PAD, depth)

    def row(j):
        return jnp.where(upward, j, rows - 1 - j)

    def span(k):
        if isinstance(k, int):
            if k == 0:
                return 0, EDGE
            if k == last:
                return width - EDGE, EDGE
        return EDGE + (k - 1) * middle, middle

    def remote(axis, to, src, dst, send, recv):
        return pltpu.make_async_remote_copy(
            src_ref=src, dst_ref=dst, send_sem=send, recv_sem=recv,
            device_id=near[axis, to], device_id_type=MESH)

    def y_face(side, p, k, from_input, to):
        start, count = span(k)
        cells, other = pl.ds(1 + start, count), 1 - side
        src = (tracer.at[side * (rows - 1), pl.ds(start, count)] if from_input
               else field[p].at[1 + side * (rows - 1), cells, inner])
        return remote("rows", to, src, field[p].at[other * (rows + 1), cells, inner],
                      y_send.at[p, side, k], y_recv.at[p, other, k])

    def z_face(side, p, k, from_input, to):
        start, count = span(k)
        cells, other, ys = pl.ds(1 + start, count), 1 - side, pl.ds(1, rows)
        src = (tracer.at[:, pl.ds(start, count), pl.ds(side * (depth - 1), 1)] if from_input
               else field[p].at[ys, cells, pl.ds(PAD + side * (depth - 1), 1)])
        return remote("slabs", to, src, field[p].at[ys, cells, pl.ds(PAD - 1 + other * (depth + 1), 1)],
                      z_send.at[p, side, k], z_recv.at[p, other, k])

    def e_face(side, p, edge, group, from_input, to):
        start, count = span(edge * last)
        cells, other = pl.ds(1 + start, count), 1 - side
        first = jnp.where(upward, group * half, rows - (group + 1) * half)
        src = (tracer.at[pl.ds(first, half), pl.ds(start, count), pl.ds(side * (depth - 1), 1)] if from_input
               else field[p].at[pl.ds(1 + first, half), cells, pl.ds(PAD + side * (depth - 1), 1)])
        dst = field[p].at[pl.ds(1 + first, half), cells, pl.ds(PAD - 1 + other * (depth + 1), 1)]
        return remote("slabs", to, src, dst, e_send.at[p, side, edge, group], e_recv.at[p, other, edge, group])

    def x_source(side, event, j, from_input):
        return (tracer.at[row(j), side * (width - 1)] if from_input
                else field[event % 2].at[1 + row(j), 1 + side * (width - 1), inner])

    def x_face(side, event, j, from_input, to):
        p, other = event % 2, 1 - side
        return remote("cols", to, x_source(side, event, j, from_input),
                      field[p].at[1 + row(j), other * (width + 1), inner],
                      x_send.at[p, side, j], x_recv.at[p, other, j])

    def first_relayed(event):
        return 0 if event % 2 == 1 else rows - share

    def first_hop(source, event, j, from_input):
        side, n = 2 - source, j - first_relayed(event)
        return pltpu.make_async_remote_copy(
            src_ref=x_source(side, event, j, from_input), dst_ref=relayed.at[event, n],
            send_sem=x_send.at[event % 2, side, j], recv_sem=r_recv.at[event, n],
            device_id={"cols": via[source]}, device_id_type=MESH)

    def second_hop(source, event, j):
        side, n, p = 2 - source, j - first_relayed(event), event % 2
        return pltpu.make_async_remote_copy(
            src_ref=relayed.at[event, n],
            dst_ref=field[p].at[1 + row(j), (1 - side) * (width + 1), inner],
            send_sem=f_send.at[event, n], recv_sem=x_recv.at[p, 1 - side, j],
            device_id={"cols": 3 - source}, device_id_type=MESH)

    def send_x(side, event, j, from_input=False):
        if not via:
            pl.when(has["cols", side])(lambda: x_face(side, event, j, from_input, side).start())
            return
        first = first_relayed(event)
        relay = jnp.logical_and(col == 2 - side, jnp.logical_and(j >= first, j < first + share))
        pl.when(relay)(lambda: first_hop(2 - side, event, j, from_input).start())
        pl.when(jnp.logical_and(has["cols", side], jnp.logical_not(relay)))(
            lambda: x_face(side, event, j, from_input, side).start())

    def forward(event, j):
        for source in (1, 2):
            @pl.when(col == via[source])
            def _():
                n = j - first_relayed(event)
                pltpu.make_async_remote_copy(
                    src_ref=relayed.at[event, n], dst_ref=relayed.at[event, n],
                    send_sem=f_send.at[event, n], recv_sem=r_recv.at[event, n],
                    device_id={"cols": 3 - source}, device_id_type=MESH).wait_recv()
                second_hop(source, event, j).start()

    def by_side(axis, action):
        for side in (0, 1):
            pl.when(has[axis, side])(functools.partial(action, side))

    tracer_parts = [(0, EDGE + 1)]
    tracer_parts += [(EDGE + k * middle + 1, middle) for k in range(slots - 1)]
    tracer_parts += [(EDGE + (slots - 1) * middle + 1, middle - 2), (width - EDGE - 1, EDGE + 1)]

    def load_tracer(k):
        start, count = tracer_parts[k]
        return pltpu.make_async_copy(
            tracer.at[:, pl.ds(start, count)],
            field[0].at[pl.ds(1, rows), pl.ds(1 + start, count), inner], load_sem.at[0, k])

    def load_limit(k):
        start, count = span(k)
        return pltpu.make_async_copy(
            crowding.at[:, pl.ds(start, count)], limit.at[:, pl.ds(start, count)], load_sem.at[1, k])

    barrier = pltpu.get_barrier_semaphore()
    for axis in AXES:
        by_side(axis, lambda side: pl.semaphore_signal(
            barrier, inc=1, device_id=near[axis, side], device_id_type=MESH))
    if via:
        pl.semaphore_signal(barrier, inc=1, device_id={"cols": lax.rem(col + 2, 4)}, device_id_type=MESH)
    for k in (0, last, 1):
        load_tracer(k).start()
    for k in (1, 0, last):
        load_limit(k).start()
    for k in range(2, last):
        load_tracer(k).start()
        load_limit(k).start()
    pl.semaphore_wait(barrier, (1 if via else 0) + sum(jnp.where(has[key], 1, 0) for key in has))

    for j in range(rows):
        for side in (0, 1):
            send_x(side, 0, j, True)
    for k in [1, 0, last, *range(2, last)]:
        by_side("rows", lambda side: y_face(side, 0, k, True, side).start())
        if k in (0, last):
            for group in range(rows // half):
                by_side("slabs", lambda side: e_face(side, 0, k // last, group, True, side).start())
        else:
            by_side("slabs", lambda side: z_face(side, 0, k, True, side).start())

    def clear(axis, side):
        @pl.when(jnp.logical_not(has[axis, side]))
        def _():
            for p in (0, 1):
                if axis == "rows":
                    @pl.loop(1, width + 1)
                    def _(x):
                        field[p][side * (rows + 1), x, inner] = jnp.zeros((depth, species), jnp.float32)
                elif axis == "cols":
                    @pl.loop(1, rows + 1)
                    def _(y):
                        field[p][y, side * (width + 1), inner] = jnp.zeros((depth, species), jnp.float32)
                else:
                    @pl.loop(1, width + 1)
                    def _(x):
                        for y in range(1, rows + 1):
                            field[p][y, x, pl.ds(PAD - 1 + side * (depth + 1), 1)] = jnp.zeros((1, species), jnp.float32)

    for axis in AXES:
        for side in (0, 1):
            clear(axis, side)

    def scale(step):
        return 0.2 if step == 0 else 0.05 if step == STEPS - 1 else 0.1

    def advance(step, k):
        p = step % 2
        start, count = span(k)

        @pl.loop(0, depth // 8)
        def _(tile):
            at = pl.multiple_of(PAD + tile * 8, 8)
            source = pl.multiple_of(tile * 8, 8)

            def cell(y, x, shift=0):
                return field[p][y, 1 + start + x, pl.ds(at + shift, 8)]

            before = [cell(y, -1) for y in range(1, rows + 1)]
            here = [cell(y, 0) for y in range(1, rows + 1)]
            for x in range(count):
                after = [cell(y, x + 1) for y in range(1, rows + 1)]
                column = [cell(0, x), *here, cell(rows + 1, x)]
                for y in range(rows):
                    here_y = here[y]
                    around = (before[y] + after[y]) + (column[y] + column[y + 2])
                    around = around + (cell(y + 1, x, -1) + cell(y + 1, x, 1))
                    bound = limit[y, start + x, pl.ds(source, 8)]
                    if step == 0:
                        bound = bound + bound
                    field[1 - p][y + 1, 1 + start + x, pl.ds(at, 8)] = scale(step) * (
                        around + here_y * (6.0 - bound * here_y))
                before, here = here, after

    def advance_edges(step, y):
        p = step % 2
        tiles = depth // 8
        group = next(g for g in (4, 3, 2, 1) if tiles % g == 0)

        @pl.loop(0, tiles // group)
        def _(block):
            for n in range(group):
                at = pl.multiple_of(PAD + block * (8 * group) + 8 * n, 8)
                source = pl.multiple_of(block * (8 * group) + 8 * n, 8)
                for edge in (0, 1):
                    start = edge * (width - EDGE)

                    def cell(x, shift=0, up=0):
                        return field[p][1 + y + up, 1 + start + x, pl.ds(at + shift, 8)]

                    line = [cell(x) for x in range(-1, EDGE + 1)]
                    for x in range(EDGE):
                        here = line[x + 1]
                        around = (line[x] + line[x + 2]) + (cell(x, 0, -1) + cell(x, 0, 1))
                        around = around + (cell(x, -1) + cell(x, 1))
                        bound = limit[y, start + x, pl.ds(source, 8)]
                        if step == 0:
                            bound = bound + bound
                        field[1 - p][1 + y, 1 + start + x, pl.ds(at, 8)] = scale(step) * (
                            around + here * (6.0 - bound * here))

    def centre(step, k):
        p = step % 2
        if step == 0:
            load_limit(k).wait()
        by_side("rows", lambda side: y_face(1 - side, p, k, False, side).wait_recv())
        by_side("slabs", lambda side: z_face(1 - side, p, k, False, side).wait_recv())
        if step >= 1:
            by_side("rows", lambda side: y_face(side, 1 - p, k, False, side).wait_send())
            by_side("slabs", lambda side: z_face(side, 1 - p, k, False, side).wait_send())
        advance(step, k)
        if step < STEPS - 1:
            by_side("rows", lambda side: y_face(side, 1 - p, k, False, side).start())
            by_side("slabs", lambda side: z_face(side, 1 - p, k, False, side).start())

    def edges(step, j):
        p = step % 2
        y = row(j)
        group = j // half

        def at_row(side):
            return jnp.logical_and(has["rows", side], y == side * (rows - 1))

        for side in (0, 1):
            @pl.when(at_row(side))
            def _():
                for k in (0, last):
                    y_face(1 - side, p, k, False, side).wait_recv()
                    if step >= 1:
                        y_face(side, 1 - p, k, False, side).wait_send()

        @pl.when(lax.rem(j, half) == 0)
        def _():
            for edge in (0, 1):
                by_side("slabs", lambda side: e_face(1 - side, p, edge, group, False, side).wait_recv())
                if step >= 1:
                    by_side("slabs", lambda side: e_face(side, 1 - p, edge, group, False, side).wait_send())

        by_side("cols", lambda side: x_face(1 - side, step, j, False, side).wait_recv())
        if step >= 1:
            by_side("cols", lambda side: x_face(side, step - 1, j, False, side).wait_send())
        advance_edges(step, y)
        if step < STEPS - 1:
            for side in (0, 1):
                send_x(side, step + 1, j)
            for side in (0, 1):
                @pl.when(at_row(side))
                def _():
                    for k in (0, last):
                        y_face(side, 1 - p, k, False, side).start()

            @pl.when(lax.rem(j, half) == half - 1)
            def _():
                for edge in (0, 1):
                    by_side("slabs", lambda side: e_face(side, 1 - p, edge, group, False, side).start())

    forwards = {}
    if via:
        for event in range(STEPS):
            for n in range(share):
                j = first_relayed(event) + n
                when = (FIRST + n) if event == 0 else (event - 1) * slots + j + LATE
                forwards.setdefault(min(when, STEPS * slots - 1), []).append((event, j))

    for step in range(STEPS):
        if step == 0:
            for k in (0, last, 1):
                load_tracer(k).wait()

        @pl.loop(0, slots)
        def _(slot):
            if step > 0:
                centre(step, slot + 1)
            if step == 0:
                for k in range(2, last):
                    pl.when(slot == k - 1)(functools.partial(lambda k: load_tracer(k).wait(), k))
                centre(step, slot + 1)

                @pl.when(slot == 0)
                def _():
                    for k in (0, last):
                        load_limit(k).wait()
            for n in range(slots):
                for event, j in forwards.get(step * slots + n, []):
                    pl.when(slot == n)(functools.partial(forward, event, j))
            edges(step, slot)

    p = (STEPS - 1) % 2

    @pl.loop(1, last)
    def _(k):
        by_side("rows", lambda side: y_face(side, p, k, False, side).wait_send())
        by_side("slabs", lambda side: z_face(side, p, k, False, side).wait_send())

    for k in (0, last):
        by_side("rows", lambda side: y_face(side, p, k, False, side).wait_send())
        for group in range(rows // half):
            by_side("slabs", lambda side: e_face(side, p, k // last, group, False, side).wait_send())
    for j in range(rows):
        by_side("cols", lambda side: x_face(side, STEPS - 1, j, False, side).wait_send())
    for when in sorted(forwards):
        for event, j in forwards[when]:
            for source in (1, 2):
                pl.when(col == via[source])(lambda: second_hop(source, event, j).wait_send())


def relays(mesh):
    if mesh.shape["cols"] != 4:
        return None
    devices = mesh.devices.transpose([mesh.axis_names.index(axis) for axis in AXES])[0, :, 0]
    chips = [getattr(device, "coords", None) for device in devices]
    if any(chip is None for chip in chips):
        return None
    apart = sum(a != b for a, b in zip(chips[1], chips[2]))
    return VIA if apart > 1 else None


def solution(mesh):
    sizes = dict(mesh.shape)
    via = relays(mesh)

    def on_device(tracer, crowding):
        rows, width, depth, species = tracer.shape
        half = rows // 2 if rows % 2 == 0 else rows
        groups, share, parts = rows // half, max(1, rows // 2), rows + 2
        dma = pltpu.SemaphoreType.DMA
        padded = (rows + 2, width + 2, depth + 2 * PAD, species)
        cell_count = rows * width * depth * species
        ended = pl.pallas_call(
            functools.partial(kernel, sizes, via),
            out_shape=pltpu.VMEM(padded, jnp.float32),
            in_specs=[pl.BlockSpec(memory_space=pl.ANY)] * 2,
            out_specs=pl.BlockSpec(memory_space=pltpu.VMEM),
            scratch_shapes=[
                pltpu.VMEM(padded, jnp.float32),
                pltpu.VMEM(tracer.shape, jnp.float32),
                dma((2, parts)),
                dma((2, 2, parts)), dma((2, 2, parts)),
                dma((2, 2, parts)), dma((2, 2, parts)),
                dma((2, 2, 2, groups)), dma((2, 2, 2, groups)),
                dma((2, 2, rows)), dma((2, 2, rows)),
                pltpu.VMEM((STEPS, share, depth, species), jnp.float32),
                dma((STEPS, share)), dma((STEPS, share)),
            ],
            compiler_params=pltpu.CompilerParams(
                collective_id=0, has_side_effects=True, vmem_limit_bytes=VMEM_LIMIT),
        )(tracer, crowding)
        return pl.pallas_call(
            write,
            out_shape=jax.ShapeDtypeStruct(tracer.shape, jnp.float32),
            in_specs=[pl.BlockSpec(memory_space=pltpu.VMEM)],
            out_specs=pl.BlockSpec(memory_space=pl.ANY),
            scratch_shapes=[dma((rows,))],
            compiler_params=pltpu.CompilerParams(vmem_limit_bytes=1 << 20),
        )(ended)

    return jax.shard_map(
        on_device, mesh=mesh,
        in_specs=(P("rows", "cols", "slabs", None), P("rows", "cols", "slabs", None)),
        out_specs=P("rows", "cols", "slabs", None), check_vma=False)
```

```python
import functools

import jax
import jax.numpy as jnp
from jax import lax
from jax.experimental import pallas as pl
from jax.experimental.pallas import tpu as pltpu
from jax.sharding import PartitionSpec as P

STEPS = 4
EDGE = 2
VIA = {1: 3, 2: 0}
LATE = 2
FIRST = 0
PAD = 8
VMEM_LIMIT = 40 * 1024 * 1024
MESH = pl.DeviceIdType.MESH
AXES = ("rows", "cols", "slabs")


def write(ended, out, store_sem):
    rows, width, depth, species = out.shape
    copies = [pltpu.make_async_copy(
        ended.at[1 + y, pl.ds(1, width), pl.ds(PAD, depth)], out.at[y], store_sem.at[y])
        for y in range(rows)]
    for copy in copies:
        copy.start()
    for copy in copies:
        copy.wait()


def kernel(sizes, via, tracer, crowding, ended, other_field, limit, load_sem,
           y_send, y_recv, z_send, z_recv, e_send, e_recv, x_send, x_recv,
           relayed, r_recv, f_send):
    rows, width, depth, species = tracer.shape
    slots = rows
    middle = (width - 2 * EDGE) // slots
    last = slots + 1
    half = rows // 2 if rows % 2 == 0 else rows
    share = rows // 2
    field = (ended, other_field)
    place = {axis: lax.axis_index(axis) for axis in AXES}
    has = {(axis, side): (place[axis] > 0) if side == 0 else (place[axis] < sizes[axis] - 1)
           for axis in AXES for side in (0, 1)}
    near = {(axis, side): {axis: jnp.clip(place[axis] + 2 * side - 1, 0, sizes[axis] - 1)}
            for axis in AXES for side in (0, 1)}
    col = place["cols"]
    upward = lax.rem(place["rows"], 2) == 1
    inner = pl.ds(PAD, depth)

    def row(j):
        return jnp.where(upward, j, rows - 1 - j)

    def span(k):
        if isinstance(k, int):
            if k == 0:
                return 0, EDGE
            if k == last:
                return width - EDGE, EDGE
        return EDGE + (k - 1) * middle, middle

    def remote(axis, to, src, dst, send, recv):
        return pltpu.make_async_remote_copy(
            src_ref=src, dst_ref=dst, send_sem=send, recv_sem=recv,
            device_id=near[axis, to], device_id_type=MESH)

    def y_face(side, p, k, from_input, to):
        start, count = span(k)
        cells, other = pl.ds(1 + start, count), 1 - side
        src = (tracer.at[side * (rows - 1), pl.ds(start, count)] if from_input
               else field[p].at[1 + side * (rows - 1), cells, inner])
        return remote("rows", to, src, field[p].at[other * (rows + 1), cells, inner],
                      y_send.at[p, side, k], y_recv.at[p, other, k])

    def z_face(side, p, k, from_input, to):
        start, count = span(k)
        cells, other, ys = pl.ds(1 + start, count), 1 - side, pl.ds(1, rows)
        src = (tracer.at[:, pl.ds(start, count), pl.ds(side * (depth - 1), 1)] if from_input
               else field[p].at[ys, cells, pl.ds(PAD + side * (depth - 1), 1)])
        return remote("slabs", to, src, field[p].at[ys, cells, pl.ds(PAD - 1 + other * (depth + 1), 1)],
                      z_send.at[p, side, k], z_recv.at[p, other, k])

    def e_face(side, p, edge, group, from_input, to):
        start, count = span(edge * last)
        cells, other = pl.ds(1 + start, count), 1 - side
        first = jnp.where(upward, group * half, rows - (group + 1) * half)
        src = (tracer.at[pl.ds(first, half), pl.ds(start, count), pl.ds(side * (depth - 1), 1)] if from_input
               else field[p].at[pl.ds(1 + first, half), cells, pl.ds(PAD + side * (depth - 1), 1)])
        dst = field[p].at[pl.ds(1 + first, half), cells, pl.ds(PAD - 1 + other * (depth + 1), 1)]
        return remote("slabs", to, src, dst, e_send.at[p, side, edge, group], e_recv.at[p, other, edge, group])

    def x_source(side, event, j, from_input):
        return (tracer.at[row(j), side * (width - 1)] if from_input
                else field[event % 2].at[1 + row(j), 1 + side * (width - 1), inner])

    def x_face(side, event, j, from_input, to):
        p, other = event % 2, 1 - side
        return remote("cols", to, x_source(side, event, j, from_input),
                      field[p].at[1 + row(j), other * (width + 1), inner],
                      x_send.at[p, side, j], x_recv.at[p, other, j])

    def first_relayed(event):
        return 0 if event % 2 == 1 else rows - share

    def first_hop(source, event, j, from_input):
        side, n = 2 - source, j - first_relayed(event)
        return pltpu.make_async_remote_copy(
            src_ref=x_source(side, event, j, from_input), dst_ref=relayed.at[event, n],
            send_sem=x_send.at[event % 2, side, j], recv_sem=r_recv.at[event, n],
            device_id={"cols": via[source]}, device_id_type=MESH)

    def second_hop(source, event, j):
        side, n, p = 2 - source, j - first_relayed(event), event % 2
        return pltpu.make_async_remote_copy(
            src_ref=relayed.at[event, n],
            dst_ref=field[p].at[1 + row(j), (1 - side) * (width + 1), inner],
            send_sem=f_send.at[event, n], recv_sem=x_recv.at[p, 1 - side, j],
            device_id={"cols": 3 - source}, device_id_type=MESH)

    def send_x(side, event, j, from_input=False):
        if not via:
            pl.when(has["cols", side])(lambda: x_face(side, event, j, from_input, side).start())
            return
        first = first_relayed(event)
        relay = jnp.logical_and(col == 2 - side, jnp.logical_and(j >= first, j < first + share))
        pl.when(relay)(lambda: first_hop(2 - side, event, j, from_input).start())
        pl.when(jnp.logical_and(has["cols", side], jnp.logical_not(relay)))(
            lambda: x_face(side, event, j, from_input, side).start())

    def forward(event, j):
        for source in (1, 2):
            @pl.when(col == via[source])
            def _():
                n = j - first_relayed(event)
                pltpu.make_async_remote_copy(
                    src_ref=relayed.at[event, n], dst_ref=relayed.at[event, n],
                    send_sem=f_send.at[event, n], recv_sem=r_recv.at[event, n],
                    device_id={"cols": 3 - source}, device_id_type=MESH).wait_recv()
                second_hop(source, event, j).start()

    def by_side(axis, action):
        for side in (0, 1):
            pl.when(has[axis, side])(functools.partial(action, side))

    tracer_parts = [(0, EDGE + 1)]
    tracer_parts += [(EDGE + k * middle + 1, middle) for k in range(slots - 1)]
    tracer_parts += [(EDGE + (slots - 1) * middle + 1, middle - 2), (width - EDGE - 1, EDGE + 1)]

    def load_tracer(k):
        start, count = tracer_parts[k]
        return pltpu.make_async_copy(
            tracer.at[:, pl.ds(start, count)],
            field[0].at[pl.ds(1, rows), pl.ds(1 + start, count), inner], load_sem.at[0, k])

    def load_limit(k):
        start, count = span(k)
        return pltpu.make_async_copy(
            crowding.at[:, pl.ds(start, count)], limit.at[:, pl.ds(start, count)], load_sem.at[1, k])

    barrier = pltpu.get_barrier_semaphore()
    for axis in AXES:
        by_side(axis, lambda side: pl.semaphore_signal(
            barrier, inc=1, device_id=near[axis, side], device_id_type=MESH))
    if via:
        pl.semaphore_signal(barrier, inc=1, device_id={"cols": lax.rem(col + 2, 4)}, device_id_type=MESH)
    for k in (0, last, 1):
        load_tracer(k).start()
    for k in (1, 0, last):
        load_limit(k).start()
    for k in range(2, last):
        load_tracer(k).start()
        load_limit(k).start()
    pl.semaphore_wait(barrier, (1 if via else 0) + sum(jnp.where(has[key], 1, 0) for key in has))

    for j in range(rows):
        for side in (0, 1):
            send_x(side, 0, j, True)
    for k in [1, 0, last, *range(2, last)]:
        by_side("rows", lambda side: y_face(side, 0, k, True, side).start())
        if k in (0, last):
            for group in range(rows // half):
                by_side("slabs", lambda side: e_face(side, 0, k // last, group, True, side).start())
        else:
            by_side("slabs", lambda side: z_face(side, 0, k, True, side).start())

    def clear(axis, side):
        @pl.when(jnp.logical_not(has[axis, side]))
        def _():
            for p in (0, 1):
                if axis == "rows":
                    @pl.loop(1, width + 1)
                    def _(x):
                        field[p][side * (rows + 1), x, inner] = jnp.zeros((depth, species), jnp.float32)
                elif axis == "cols":
                    @pl.loop(1, rows + 1)
                    def _(y):
                        field[p][y, side * (width + 1), inner] = jnp.zeros((depth, species), jnp.float32)
                else:
                    @pl.loop(1, width + 1)
                    def _(x):
                        for y in range(1, rows + 1):
                            field[p][y, x, pl.ds(PAD - 1 + side * (depth + 1), 1)] = jnp.zeros((1, species), jnp.float32)

    for axis in AXES:
        for side in (0, 1):
            clear(axis, side)

    def scale(step):
        return 0.2 if step == 0 else 0.05 if step == STEPS - 1 else 0.1

    def advance(step, k):
        p = step % 2
        start, count = span(k)

        @pl.loop(0, depth // 8)
        def _(tile):
            at = pl.multiple_of(PAD + tile * 8, 8)
            source = pl.multiple_of(tile * 8, 8)

            def cell(y, x, shift=0):
                return field[p][y, 1 + start + x, pl.ds(at + shift, 8)]

            here = [cell(y, 0) for y in range(rows + 2)]
            slant = [cell(y, -1) + here[y + 1] for y in range(1, rows + 1)]
            for x in range(count):
                after = [None, *[cell(y, x + 1) for y in range(1, rows + 1)], None]
                steep = [here[y] + after[y + 1] for y in range(rows)]
                for y in range(rows):
                    here_y = here[y + 1]
                    around = (slant[y] + steep[y]) + (cell(y + 1, x, -1) + cell(y + 1, x, 1))
                    bound = limit[y, start + x, pl.ds(source, 8)]
                    if step == 0:
                        bound = bound + bound
                    field[1 - p][y + 1, 1 + start + x, pl.ds(at, 8)] = scale(step) * (
                        around + here_y * (6.0 - bound * here_y))
                if x < count - 1:
                    after[0], after[-1] = cell(0, x + 1), cell(rows + 1, x + 1)
                    slant = [*steep[1:], here[rows] + after[rows + 1]]
                    here = after

    def advance_edges(step, y):
        p = step % 2
        tiles = depth // 8
        group = next(g for g in (4, 3, 2, 1) if tiles % g == 0)

        @pl.loop(0, tiles // group)
        def _(block):
            for n in range(group):
                at = pl.multiple_of(PAD + block * (8 * group) + 8 * n, 8)
                source = pl.multiple_of(block * (8 * group) + 8 * n, 8)
                for edge in (0, 1):
                    start = edge * (width - EDGE)

                    def cell(x, shift=0, up=0):
                        return field[p][1 + y + up, 1 + start + x, pl.ds(at + shift, 8)]

                    line = [cell(x) for x in range(-1, EDGE + 1)]
                    for x in range(EDGE):
                        here = line[x + 1]
                        around = (line[x] + line[x + 2]) + (cell(x, 0, -1) + cell(x, 0, 1))
                        around = around + (cell(x, -1) + cell(x, 1))
                        bound = limit[y, start + x, pl.ds(source, 8)]
                        if step == 0:
                            bound = bound + bound
                        field[1 - p][1 + y, 1 + start + x, pl.ds(at, 8)] = scale(step) * (
                            around + here * (6.0 - bound * here))

    def centre(step, k):
        p = step % 2
        if step == 0:
            load_limit(k).wait()
        by_side("rows", lambda side: y_face(1 - side, p, k, False, side).wait_recv())
        by_side("slabs", lambda side: z_face(1 - side, p, k, False, side).wait_recv())
        if step >= 1:
            by_side("rows", lambda side: y_face(side, 1 - p, k, False, side).wait_send())
            by_side("slabs", lambda side: z_face(side, 1 - p, k, False, side).wait_send())
        advance(step, k)
        if step < STEPS - 1:
            by_side("rows", lambda side: y_face(side, 1 - p, k, False, side).start())
            by_side("slabs", lambda side: z_face(side, 1 - p, k, False, side).start())

    def edges(step, j):
        p = step % 2
        y = row(j)
        group = j // half

        def at_row(side):
            return jnp.logical_and(has["rows", side], y == side * (rows - 1))

        for side in (0, 1):
            @pl.when(at_row(side))
            def _():
                for k in (0, last):
                    y_face(1 - side, p, k, False, side).wait_recv()
                    if step >= 1:
                        y_face(side, 1 - p, k, False, side).wait_send()

        @pl.when(lax.rem(j, half) == 0)
        def _():
            for edge in (0, 1):
                by_side("slabs", lambda side: e_face(1 - side, p, edge, group, False, side).wait_recv())
                if step >= 1:
                    by_side("slabs", lambda side: e_face(side, 1 - p, edge, group, False, side).wait_send())

        by_side("cols", lambda side: x_face(1 - side, step, j, False, side).wait_recv())
        if step >= 1:
            by_side("cols", lambda side: x_face(side, step - 1, j, False, side).wait_send())
        advance_edges(step, y)
        if step < STEPS - 1:
            for side in (0, 1):
                send_x(side, step + 1, j)
            for side in (0, 1):
                @pl.when(at_row(side))
                def _():
                    for k in (0, last):
                        y_face(side, 1 - p, k, False, side).start()

            @pl.when(lax.rem(j, half) == half - 1)
            def _():
                for edge in (0, 1):
                    by_side("slabs", lambda side: e_face(side, 1 - p, edge, group, False, side).start())

    forwards = {}
    if via:
        for event in range(STEPS):
            for n in range(share):
                j = first_relayed(event) + n
                when = (FIRST + n) if event == 0 else (event - 1) * slots + j + LATE
                forwards.setdefault(min(when, STEPS * slots - 1), []).append((event, j))

    for step in range(STEPS):
        if step == 0:
            for k in (0, last, 1):
                load_tracer(k).wait()

        @pl.loop(0, slots)
        def _(slot):
            if step > 0:
                centre(step, slot + 1)
            if step == 0:
                for k in range(2, last):
                    pl.when(slot == k - 1)(functools.partial(lambda k: load_tracer(k).wait(), k))
                centre(step, slot + 1)

                @pl.when(slot == 0)
                def _():
                    for k in (0, last):
                        load_limit(k).wait()
            for n in range(slots):
                for event, j in forwards.get(step * slots + n, []):
                    pl.when(slot == n)(functools.partial(forward, event, j))
            edges(step, slot)

    p = (STEPS - 1) % 2

    @pl.loop(1, last)
    def _(k):
        by_side("rows", lambda side: y_face(side, p, k, False, side).wait_send())
        by_side("slabs", lambda side: z_face(side, p, k, False, side).wait_send())

    for k in (0, last):
        by_side("rows", lambda side: y_face(side, p, k, False, side).wait_send())
        for group in range(rows // half):
            by_side("slabs", lambda side: e_face(side, p, k // last, group, False, side).wait_send())
    for j in range(rows):
        by_side("cols", lambda side: x_face(side, STEPS - 1, j, False, side).wait_send())
    for when in sorted(forwards):
        for event, j in forwards[when]:
            for source in (1, 2):
                pl.when(col == via[source])(lambda: second_hop(source, event, j).wait_send())


def relays(mesh):
    if mesh.shape["cols"] != 4:
        return None
    devices = mesh.devices.transpose([mesh.axis_names.index(axis) for axis in AXES])[0, :, 0]
    chips = [getattr(device, "coords", None) for device in devices]
    if any(chip is None for chip in chips):
        return None
    apart = sum(a != b for a, b in zip(chips[1], chips[2]))
    return VIA if apart > 1 else None


def solution(mesh):
    sizes = dict(mesh.shape)
    via = relays(mesh)

    def on_device(tracer, crowding):
        rows, width, depth, species = tracer.shape
        half = rows // 2 if rows % 2 == 0 else rows
        groups, share, parts = rows // half, max(1, rows // 2), rows + 2
        dma = pltpu.SemaphoreType.DMA
        padded = (rows + 2, width + 2, depth + 2 * PAD, species)
        cell_count = rows * width * depth * species
        ended = pl.pallas_call(
            functools.partial(kernel, sizes, via),
            out_shape=pltpu.VMEM(padded, jnp.float32),
            in_specs=[pl.BlockSpec(memory_space=pl.ANY)] * 2,
            out_specs=pl.BlockSpec(memory_space=pltpu.VMEM),
            scratch_shapes=[
                pltpu.VMEM(padded, jnp.float32),
                pltpu.VMEM(tracer.shape, jnp.float32),
                dma((2, parts)),
                dma((2, 2, parts)), dma((2, 2, parts)),
                dma((2, 2, parts)), dma((2, 2, parts)),
                dma((2, 2, 2, groups)), dma((2, 2, 2, groups)),
                dma((2, 2, rows)), dma((2, 2, rows)),
                pltpu.VMEM((STEPS, share, depth, species), jnp.float32),
                dma((STEPS, share)), dma((STEPS, share)),
            ],
            compiler_params=pltpu.CompilerParams(
                collective_id=0, has_side_effects=True, vmem_limit_bytes=VMEM_LIMIT),
        )(tracer, crowding)
        return pl.pallas_call(
            write,
            out_shape=jax.ShapeDtypeStruct(tracer.shape, jnp.float32),
            in_specs=[pl.BlockSpec(memory_space=pltpu.VMEM)],
            out_specs=pl.BlockSpec(memory_space=pl.ANY),
            scratch_shapes=[dma((rows,))],
            compiler_params=pltpu.CompilerParams(vmem_limit_bytes=1 << 20),
        )(ended)

    return jax.shard_map(
        on_device, mesh=mesh,
        in_specs=(P("rows", "cols", "slabs", None), P("rows", "cols", "slabs", None)),
        out_specs=P("rows", "cols", "slabs", None), check_vma=False)
```

```python
import functools

import jax
import jax.numpy as jnp
from jax import lax
from jax.experimental import pallas as pl
from jax.experimental.pallas import tpu as pltpu
from jax.sharding import PartitionSpec as P

STEPS = 4
EDGE = 2
VIA = {1: 3, 2: 0}
LATE = 2
FIRST = 0
PAD = 8
TAIL = 2
RING = 8
MESH = pl.DeviceIdType.MESH
AXES = ("rows", "cols", "slabs")


def scale(step):
    return 0.2 if step == 0 else 0.05 if step == STEPS - 1 else 0.1


def stencil(step, now, limit, rows, depth, start, count, store):
    @pl.loop(0, depth // 8)
    def _(tile):
        source = pl.multiple_of(tile * 8, 8)
        at = pl.multiple_of(PAD + tile * 8, 8)

        def cell(y, x, shift=0):
            return now[y, 1 + start + x, pl.ds(at + shift, 8)]

        here = [cell(y, 0) for y in range(rows + 2)]
        slant = [cell(y, -1) + here[y + 1] for y in range(1, rows + 1)]
        for x in range(count):
            after = [None, *[cell(y, x + 1) for y in range(1, rows + 1)], None]
            steep = [here[y] + after[y + 1] for y in range(rows)]
            for y in range(rows):
                middle = here[y + 1]
                around = (slant[y] + steep[y]) + (cell(y + 1, x, -1) + cell(y + 1, x, 1))
                bound = limit[y, start + x, pl.ds(source, 8)]
                if step == 0:
                    bound = bound + bound
                store(x, y, source, scale(step) * (around + middle * (6.0 - bound * middle)))
            if x < count - 1:
                after[0], after[-1] = cell(0, x + 1), cell(rows + 1, x + 1)
                slant = [*steep[1:], here[rows] + after[rows + 1]]
                here = after


def tail_start(rows, width):
    middle = (width - 2 * EDGE) // rows
    return EDGE + (rows - TAIL) * middle


def write(held, out, stage, store_sem, stage_sem):
    rows, width, depth, species = out.shape
    field = held.at[pl.ds(0, rows + 2)]
    limit = held.at[pl.ds(rows + 2, rows), pl.ds(0, width), pl.ds(0, depth)]
    first, end = tail_start(rows, width), width - EDGE
    ready = [pltpu.make_async_copy(
        limit.at[y, pl.ds(start, count)], out.at[y, pl.ds(start, count)], store_sem.at[y, n])
        for n, (start, count) in enumerate(((0, first), (end, EDGE))) for y in range(rows)]
    for copy in ready:
        copy.start()
    slots, _, piece = stage.shape[:3]
    copies = []
    for n in range((end - first) // piece):
        start, slot = first + n * piece, n % slots
        if n >= slots:
            copies[n - slots].wait()

        def store(x, y, at, value):
            stage[slot, y, x, pl.ds(at, 8)] = value

        stencil(STEPS - 1, field, limit, rows, depth, start, piece, store)
        copies.append(pltpu.make_async_copy(
            stage.at[slot], out.at[:, pl.ds(start, piece)], stage_sem.at[n]))
        copies[n].start()
    for copy in [*ready, *copies[max(0, len(copies) - slots):]]:
        copy.wait()


def kernel(sizes, via, tracer, crowding, held, even_field, load_sem,
           y_send, y_recv, z_send, z_recv, e_send, e_recv, x_send, x_recv,
           relayed, r_recv, f_send):
    rows, width, depth, species = tracer.shape
    slots = rows
    middle = (width - 2 * EDGE) // slots
    last = slots + 1
    half = rows // 2 if rows % 2 == 0 else rows
    share = rows // 2
    odd_field = held.at[pl.ds(0, rows + 2)]
    limit = held.at[pl.ds(rows + 2, rows), pl.ds(0, width), pl.ds(0, depth)]
    field = (even_field, odd_field)
    place = {axis: lax.axis_index(axis) for axis in AXES}
    has = {(axis, side): (place[axis] > 0) if side == 0 else (place[axis] < sizes[axis] - 1)
           for axis in AXES for side in (0, 1)}
    near = {(axis, side): {axis: jnp.clip(place[axis] + 2 * side - 1, 0, sizes[axis] - 1)}
            for axis in AXES for side in (0, 1)}
    col = place["cols"]
    upward = lax.rem(place["rows"], 2) == 1
    inner = pl.ds(PAD, depth)

    def row(j):
        return jnp.where(upward, j, rows - 1 - j)

    def span(k):
        if isinstance(k, int):
            if k == 0:
                return 0, EDGE
            if k == last:
                return width - EDGE, EDGE
        return EDGE + (k - 1) * middle, middle

    def remote(axis, to, src, dst, send, recv):
        return pltpu.make_async_remote_copy(
            src_ref=src, dst_ref=dst, send_sem=send, recv_sem=recv,
            device_id=near[axis, to], device_id_type=MESH)

    def y_face(side, p, k, from_input, to):
        start, count = span(k)
        cells, other = pl.ds(1 + start, count), 1 - side
        src = (tracer.at[side * (rows - 1), pl.ds(start, count)] if from_input
               else field[p].at[1 + side * (rows - 1), cells, inner])
        return remote("rows", to, src, field[p].at[other * (rows + 1), cells, inner],
                      y_send.at[p, side, k], y_recv.at[p, other, k])

    def z_face(side, p, k, from_input, to):
        start, count = span(k)
        cells, other, ys = pl.ds(1 + start, count), 1 - side, pl.ds(1, rows)
        src = (tracer.at[:, pl.ds(start, count), pl.ds(side * (depth - 1), 1)] if from_input
               else field[p].at[ys, cells, pl.ds(PAD + side * (depth - 1), 1)])
        return remote("slabs", to, src, field[p].at[ys, cells, pl.ds(PAD - 1 + other * (depth + 1), 1)],
                      z_send.at[p, side, k], z_recv.at[p, other, k])

    def e_face(side, p, edge, group, from_input, to):
        start, count = span(edge * last)
        cells, other = pl.ds(1 + start, count), 1 - side
        first = jnp.where(upward, group * half, rows - (group + 1) * half)
        src = (tracer.at[pl.ds(first, half), pl.ds(start, count), pl.ds(side * (depth - 1), 1)] if from_input
               else field[p].at[pl.ds(1 + first, half), cells, pl.ds(PAD + side * (depth - 1), 1)])
        dst = field[p].at[pl.ds(1 + first, half), cells, pl.ds(PAD - 1 + other * (depth + 1), 1)]
        return remote("slabs", to, src, dst, e_send.at[p, side, edge, group], e_recv.at[p, other, edge, group])

    def x_source(side, event, j, from_input):
        return (tracer.at[row(j), side * (width - 1)] if from_input
                else field[event % 2].at[1 + row(j), 1 + side * (width - 1), inner])

    def x_face(side, event, j, from_input, to):
        p, other = event % 2, 1 - side
        return remote("cols", to, x_source(side, event, j, from_input),
                      field[p].at[1 + row(j), other * (width + 1), inner],
                      x_send.at[p, side, j], x_recv.at[p, other, j])

    def first_relayed(event):
        return 0 if event % 2 == 1 else rows - share

    def first_hop(source, event, j, from_input):
        side, n = 2 - source, j - first_relayed(event)
        return pltpu.make_async_remote_copy(
            src_ref=x_source(side, event, j, from_input), dst_ref=relayed.at[event, n],
            send_sem=x_send.at[event % 2, side, j], recv_sem=r_recv.at[event, n],
            device_id={"cols": via[source]}, device_id_type=MESH)

    def second_hop(source, event, j):
        side, n, p = 2 - source, j - first_relayed(event), event % 2
        return pltpu.make_async_remote_copy(
            src_ref=relayed.at[event, n],
            dst_ref=field[p].at[1 + row(j), (1 - side) * (width + 1), inner],
            send_sem=f_send.at[event, n], recv_sem=x_recv.at[p, 1 - side, j],
            device_id={"cols": 3 - source}, device_id_type=MESH)

    def send_x(side, event, j, from_input=False):
        if not via:
            pl.when(has["cols", side])(lambda: x_face(side, event, j, from_input, side).start())
            return
        first = first_relayed(event)
        relay = jnp.logical_and(col == 2 - side, jnp.logical_and(j >= first, j < first + share))
        pl.when(relay)(lambda: first_hop(2 - side, event, j, from_input).start())
        pl.when(jnp.logical_and(has["cols", side], jnp.logical_not(relay)))(
            lambda: x_face(side, event, j, from_input, side).start())

    def forward(event, j):
        for source in (1, 2):
            @pl.when(col == via[source])
            def _():
                n = j - first_relayed(event)
                pltpu.make_async_remote_copy(
                    src_ref=relayed.at[event, n], dst_ref=relayed.at[event, n],
                    send_sem=f_send.at[event, n], recv_sem=r_recv.at[event, n],
                    device_id={"cols": 3 - source}, device_id_type=MESH).wait_recv()
                second_hop(source, event, j).start()

    def by_side(axis, action):
        for side in (0, 1):
            pl.when(has[axis, side])(functools.partial(action, side))

    tracer_parts = [(0, EDGE + 1)]
    tracer_parts += [(EDGE + k * middle + 1, middle) for k in range(slots - 1)]
    tracer_parts += [(EDGE + (slots - 1) * middle + 1, middle - 2), (width - EDGE - 1, EDGE + 1)]

    def load_tracer(k):
        start, count = tracer_parts[k]
        return pltpu.make_async_copy(
            tracer.at[:, pl.ds(start, count)],
            field[0].at[pl.ds(1, rows), pl.ds(1 + start, count), inner], load_sem.at[0, k])

    def load_limit(k):
        start, count = span(k)
        return pltpu.make_async_copy(
            crowding.at[:, pl.ds(start, count)], limit.at[:, pl.ds(start, count)], load_sem.at[1, k])

    barrier = pltpu.get_barrier_semaphore()
    for axis in AXES:
        by_side(axis, lambda side: pl.semaphore_signal(
            barrier, inc=1, device_id=near[axis, side], device_id_type=MESH))
    if via:
        pl.semaphore_signal(barrier, inc=1, device_id={"cols": lax.rem(col + 2, 4)}, device_id_type=MESH)
    for k in (0, last, 1):
        load_tracer(k).start()
    for k in (1, 0, last):
        load_limit(k).start()
    for k in range(2, last):
        load_tracer(k).start()
        load_limit(k).start()
    pl.semaphore_wait(barrier, (1 if via else 0) + sum(jnp.where(has[key], 1, 0) for key in has))

    for j in range(rows):
        for side in (0, 1):
            send_x(side, 0, j, True)
    for k in [1, 0, last, *range(2, last)]:
        by_side("rows", lambda side: y_face(side, 0, k, True, side).start())
        if k in (0, last):
            for group in range(rows // half):
                by_side("slabs", lambda side: e_face(side, 0, k // last, group, True, side).start())
        else:
            by_side("slabs", lambda side: z_face(side, 0, k, True, side).start())

    def clear(axis, side):
        @pl.when(jnp.logical_not(has[axis, side]))
        def _():
            for p in (0, 1):
                if axis == "rows":
                    @pl.loop(1, width + 1)
                    def _(x):
                        field[p][side * (rows + 1), x, inner] = jnp.zeros((depth, species), jnp.float32)
                elif axis == "cols":
                    @pl.loop(1, rows + 1)
                    def _(y):
                        field[p][y, side * (width + 1), inner] = jnp.zeros((depth, species), jnp.float32)
                else:
                    @pl.loop(1, width + 1)
                    def _(x):
                        for y in range(1, rows + 1):
                            field[p][y, x, pl.ds(PAD - 1 + side * (depth + 1), 1)] = jnp.zeros((1, species), jnp.float32)

    for axis in AXES:
        for side in (0, 1):
            clear(axis, side)

    def advance(step, k):
        p = step % 2
        start, count = span(k)

        def store(x, y, at, value):
            if step == STEPS - 1:
                limit[y, start + x, pl.ds(at, 8)] = value
            else:
                field[1 - p][y + 1, 1 + start + x, pl.ds(PAD + at, 8)] = value

        stencil(step, field[p], limit, rows, depth, start, count, store)

    def advance_edges(step, y):
        p = step % 2
        tiles = depth // 8
        group = next(g for g in (4, 3, 2, 1) if tiles % g == 0)

        @pl.loop(0, tiles // group)
        def _(block):
            for n in range(group):
                at = pl.multiple_of(PAD + block * (8 * group) + 8 * n, 8)
                source = pl.multiple_of(block * (8 * group) + 8 * n, 8)
                for edge in (0, 1):
                    start = edge * (width - EDGE)

                    def cell(x, shift=0, up=0):
                        return field[p][1 + y + up, 1 + start + x, pl.ds(at + shift, 8)]

                    line = [cell(x) for x in range(-1, EDGE + 1)]
                    for x in range(EDGE):
                        here = line[x + 1]
                        around = (line[x] + line[x + 2]) + (cell(x, 0, -1) + cell(x, 0, 1))
                        around = around + (cell(x, -1) + cell(x, 1))
                        bound = limit[y, start + x, pl.ds(source, 8)]
                        if step == 0:
                            bound = bound + bound
                        value = scale(step) * (around + here * (6.0 - bound * here))
                        if step == STEPS - 1:
                            limit[y, start + x, pl.ds(source, 8)] = value
                        else:
                            field[1 - p][1 + y, 1 + start + x, pl.ds(at, 8)] = value

    def centre(step, k):
        p = step % 2
        if step == 0:
            load_limit(k).wait()
        by_side("rows", lambda side: y_face(1 - side, p, k, False, side).wait_recv())
        by_side("slabs", lambda side: z_face(1 - side, p, k, False, side).wait_recv())
        if step >= 1:
            by_side("rows", lambda side: y_face(side, 1 - p, k, False, side).wait_send())
            by_side("slabs", lambda side: z_face(side, 1 - p, k, False, side).wait_send())
        if step == STEPS - 1:
            pl.when(k <= slots - TAIL)(lambda: advance(step, k))
        else:
            advance(step, k)
        if step < STEPS - 1:
            by_side("rows", lambda side: y_face(side, 1 - p, k, False, side).start())
            by_side("slabs", lambda side: z_face(side, 1 - p, k, False, side).start())

    def edges(step, j):
        p = step % 2
        y = row(j)
        group = j // half

        def at_row(side):
            return jnp.logical_and(has["rows", side], y == side * (rows - 1))

        for side in (0, 1):
            @pl.when(at_row(side))
            def _():
                for k in (0, last):
                    y_face(1 - side, p, k, False, side).wait_recv()
                    if step >= 1:
                        y_face(side, 1 - p, k, False, side).wait_send()

        @pl.when(lax.rem(j, half) == 0)
        def _():
            for edge in (0, 1):
                by_side("slabs", lambda side: e_face(1 - side, p, edge, group, False, side).wait_recv())
                if step >= 1:
                    by_side("slabs", lambda side: e_face(side, 1 - p, edge, group, False, side).wait_send())

        by_side("cols", lambda side: x_face(1 - side, step, j, False, side).wait_recv())
        if step >= 1:
            by_side("cols", lambda side: x_face(side, step - 1, j, False, side).wait_send())
        advance_edges(step, y)
        if step < STEPS - 1:
            for side in (0, 1):
                send_x(side, step + 1, j)
            for side in (0, 1):
                @pl.when(at_row(side))
                def _():
                    for k in (0, last):
                        y_face(side, 1 - p, k, False, side).start()

            @pl.when(lax.rem(j, half) == half - 1)
            def _():
                for edge in (0, 1):
                    by_side("slabs", lambda side: e_face(side, 1 - p, edge, group, False, side).start())

    forwards = {}
    if via:
        for event in range(STEPS):
            for n in range(share):
                j = first_relayed(event) + n
                when = (FIRST + n) if event == 0 else (event - 1) * slots + j + LATE
                forwards.setdefault(min(when, STEPS * slots - 1), []).append((event, j))

    for step in range(STEPS):
        if step == 0:
            for k in (0, last, 1):
                load_tracer(k).wait()

        @pl.loop(0, slots)
        def _(slot):
            if step > 0:
                centre(step, slot + 1)
            if step == 0:
                for k in range(2, last):
                    pl.when(slot == k - 1)(functools.partial(lambda k: load_tracer(k).wait(), k))
                centre(step, slot + 1)

                @pl.when(slot == 0)
                def _():
                    for k in (0, last):
                        load_limit(k).wait()
            for n in range(slots):
                for event, j in forwards.get(step * slots + n, []):
                    pl.when(slot == n)(functools.partial(forward, event, j))
            edges(step, slot)

    p = (STEPS - 1) % 2

    @pl.loop(1, last)
    def _(k):
        by_side("rows", lambda side: y_face(side, p, k, False, side).wait_send())
        by_side("slabs", lambda side: z_face(side, p, k, False, side).wait_send())

    for k in (0, last):
        by_side("rows", lambda side: y_face(side, p, k, False, side).wait_send())
        for group in range(rows // half):
            by_side("slabs", lambda side: e_face(side, p, k // last, group, False, side).wait_send())
    for j in range(rows):
        by_side("cols", lambda side: x_face(side, STEPS - 1, j, False, side).wait_send())
    for when in sorted(forwards):
        for event, j in forwards[when]:
            for source in (1, 2):
                pl.when(col == via[source])(lambda: second_hop(source, event, j).wait_send())


def relays(mesh):
    if mesh.shape["cols"] != 4:
        return None
    devices = mesh.devices.transpose([mesh.axis_names.index(axis) for axis in AXES])[0, :, 0]
    chips = [getattr(device, "coords", None) for device in devices]
    if any(chip is None for chip in chips):
        return None
    apart = sum(a != b for a, b in zip(chips[1], chips[2]))
    return VIA if apart > 1 else None


def solution(mesh):
    sizes = dict(mesh.shape)
    via = relays(mesh)

    def on_device(tracer, crowding):
        rows, width, depth, species = tracer.shape
        half = rows // 2 if rows % 2 == 0 else rows
        groups, share, parts = rows // half, max(1, rows // 2), rows + 2
        dma = pltpu.SemaphoreType.DMA
        padded = (rows + 2, width + 2, depth + 2 * PAD, species)
        vmem = pl.BlockSpec(memory_space=pltpu.VMEM)
        held = pl.pallas_call(
            functools.partial(kernel, sizes, via),
            out_shape=pltpu.VMEM((2 * rows + 2, *padded[1:]), jnp.float32),
            in_specs=[pl.BlockSpec(memory_space=pl.ANY)] * 2,
            out_specs=vmem,
            scratch_shapes=[
                pltpu.VMEM(padded, jnp.float32),
                dma((2, parts)),
                dma((2, 2, parts)), dma((2, 2, parts)),
                dma((2, 2, parts)), dma((2, 2, parts)),
                dma((2, 2, 2, groups)), dma((2, 2, 2, groups)),
                dma((2, 2, rows)), dma((2, 2, rows)),
                pltpu.VMEM((STEPS, share, depth, species), jnp.float32),
                dma((STEPS, share)), dma((STEPS, share)),
            ],
            compiler_params=pltpu.CompilerParams(
                collective_id=0, has_side_effects=True, vmem_limit_bytes=23 << 20),
        )(tracer, crowding)
        piece = next(n for n in (5, 6, 4, 3, 2, 1) if (width - 2 * EDGE) // rows % n == 0)
        return pl.pallas_call(
            write,
            out_shape=jax.ShapeDtypeStruct(tracer.shape, jnp.float32),
            in_specs=[vmem],
            out_specs=pl.BlockSpec(memory_space=pl.ANY),
            scratch_shapes=[pltpu.VMEM((RING, rows, piece, depth, species), jnp.float32),
                            dma((rows, 2)), dma((max(1, width // piece),))],
            compiler_params=pltpu.CompilerParams(vmem_limit_bytes=9 << 20),
        )(held)

    return jax.shard_map(
        on_device, mesh=mesh,
        in_specs=(P("rows", "cols", "slabs", None), P("rows", "cols", "slabs", None)),
        out_specs=P("rows", "cols", "slabs", None), check_vma=False)
```

```python
import functools

import jax
import jax.numpy as jnp
from jax import lax
from jax.experimental import pallas as pl
from jax.experimental.pallas import tpu as pltpu
from jax.sharding import PartitionSpec as P

STEPS = 4
EDGE = 2
VIA = {1: 3, 2: 0}
LATE = 1
FIRST = 0
PAD = 8
TAIL = 2
RING = 8
MESH = pl.DeviceIdType.MESH
AXES = ("rows", "cols", "slabs")


def scale(step):
    return 0.2 if step == 0 else 0.05 if step == STEPS - 1 else 0.1


def stencil(step, now, limit, rows, depth, start, count, store):
    @pl.loop(0, depth // 8)
    def _(tile):
        source = pl.multiple_of(tile * 8, 8)
        at = pl.multiple_of(PAD + tile * 8, 8)

        def cell(y, x, shift=0):
            return now[y, 1 + start + x, pl.ds(at + shift, 8)]

        here = [cell(y, 0) for y in range(rows + 2)]
        slant = [cell(y, -1) + here[y + 1] for y in range(1, rows + 1)]
        for x in range(count):
            after = [None, *[cell(y, x + 1) for y in range(1, rows + 1)], None]
            steep = [here[y] + after[y + 1] for y in range(rows)]
            for y in range(rows):
                middle = here[y + 1]
                around = (slant[y] + steep[y]) + (cell(y + 1, x, -1) + cell(y + 1, x, 1))
                bound = limit[y, start + x, pl.ds(source, 8)]
                if step == 0:
                    bound = bound + bound
                store(x, y, source, scale(step) * (around + middle * (6.0 - bound * middle)))
            if x < count - 1:
                after[0], after[-1] = cell(0, x + 1), cell(rows + 1, x + 1)
                slant = [*steep[1:], here[rows] + after[rows + 1]]
                here = after


def tail_start(rows, width):
    middle = (width - 2 * EDGE) // rows
    return EDGE + (rows - TAIL) * middle


def write(held, out, stage, store_sem, stage_sem):
    rows, width, depth, species = out.shape
    field = held.at[pl.ds(0, rows + 2)]
    limit = held.at[pl.ds(rows + 2, rows), pl.ds(0, width), pl.ds(0, depth)]
    first, end = tail_start(rows, width), width - EDGE
    ready = [pltpu.make_async_copy(
        limit.at[y, pl.ds(start, count)], out.at[y, pl.ds(start, count)], store_sem.at[y, n])
        for n, (start, count) in enumerate(((0, first), (end, EDGE))) for y in range(rows)]
    for copy in ready:
        copy.start()
    slots, _, piece = stage.shape[:3]
    copies = []
    for n in range((end - first) // piece):
        start, slot = first + n * piece, n % slots
        if n >= slots:
            copies[n - slots].wait()

        def store(x, y, at, value):
            stage[slot, y, x, pl.ds(at, 8)] = value

        stencil(STEPS - 1, field, limit, rows, depth, start, piece, store)
        copies.append(pltpu.make_async_copy(
            stage.at[slot], out.at[:, pl.ds(start, piece)], stage_sem.at[n]))
        copies[n].start()
    for copy in [*ready, *copies[max(0, len(copies) - slots):]]:
        copy.wait()


def kernel(sizes, via, tracer, crowding, held, even_field, load_sem,
           y_send, y_recv, z_send, z_recv, e_send, e_recv, x_send, x_recv,
           relayed, r_recv, f_send):
    rows, width, depth, species = tracer.shape
    slots = rows
    middle = (width - 2 * EDGE) // slots
    last = slots + 1
    half = rows // 2 if rows % 2 == 0 else rows
    share = rows // 2
    odd_field = held.at[pl.ds(0, rows + 2)]
    limit = held.at[pl.ds(rows + 2, rows), pl.ds(0, width), pl.ds(0, depth)]
    field = (even_field, odd_field)
    place = {axis: lax.axis_index(axis) for axis in AXES}
    has = {(axis, side): (place[axis] > 0) if side == 0 else (place[axis] < sizes[axis] - 1)
           for axis in AXES for side in (0, 1)}
    near = {(axis, side): {axis: jnp.clip(place[axis] + 2 * side - 1, 0, sizes[axis] - 1)}
            for axis in AXES for side in (0, 1)}
    col = place["cols"]
    upward = lax.rem(place["rows"], 2) == 1
    inner = pl.ds(PAD, depth)

    def row(j):
        return jnp.where(upward, j, rows - 1 - j)

    def span(k):
        if isinstance(k, int):
            if k == 0:
                return 0, EDGE
            if k == last:
                return width - EDGE, EDGE
        return EDGE + (k - 1) * middle, middle

    def remote(axis, to, src, dst, send, recv):
        return pltpu.make_async_remote_copy(
            src_ref=src, dst_ref=dst, send_sem=send, recv_sem=recv,
            device_id=near[axis, to], device_id_type=MESH)

    def y_face(side, p, k, from_input, to):
        start, count = span(k)
        cells, other = pl.ds(1 + start, count), 1 - side
        src = (tracer.at[side * (rows - 1), pl.ds(start, count)] if from_input
               else field[p].at[1 + side * (rows - 1), cells, inner])
        return remote("rows", to, src, field[p].at[other * (rows + 1), cells, inner],
                      y_send.at[p, side, k], y_recv.at[p, other, k])

    def z_face(side, p, k, from_input, to):
        start, count = span(k)
        cells, other, ys = pl.ds(1 + start, count), 1 - side, pl.ds(1, rows)
        src = (tracer.at[:, pl.ds(start, count), pl.ds(side * (depth - 1), 1)] if from_input
               else field[p].at[ys, cells, pl.ds(PAD + side * (depth - 1), 1)])
        return remote("slabs", to, src, field[p].at[ys, cells, pl.ds(PAD - 1 + other * (depth + 1), 1)],
                      z_send.at[p, side, k], z_recv.at[p, other, k])

    def e_face(side, p, edge, group, from_input, to):
        start, count = span(edge * last)
        cells, other = pl.ds(1 + start, count), 1 - side
        first = jnp.where(upward, group * half, rows - (group + 1) * half)
        src = (tracer.at[pl.ds(first, half), pl.ds(start, count), pl.ds(side * (depth - 1), 1)] if from_input
               else field[p].at[pl.ds(1 + first, half), cells, pl.ds(PAD + side * (depth - 1), 1)])
        dst = field[p].at[pl.ds(1 + first, half), cells, pl.ds(PAD - 1 + other * (depth + 1), 1)]
        return remote("slabs", to, src, dst, e_send.at[p, side, edge, group], e_recv.at[p, other, edge, group])

    def x_source(side, event, j, from_input):
        return (tracer.at[row(j), side * (width - 1)] if from_input
                else field[event % 2].at[1 + row(j), 1 + side * (width - 1), inner])

    def x_face(side, event, j, from_input, to):
        p, other = event % 2, 1 - side
        return remote("cols", to, x_source(side, event, j, from_input),
                      field[p].at[1 + row(j), other * (width + 1), inner],
                      x_send.at[p, side, j], x_recv.at[p, other, j])

    def first_relayed(event):
        return 0 if event % 2 == 1 else rows - share

    def first_hop(source, event, j, from_input):
        side, n = 2 - source, j - first_relayed(event)
        return pltpu.make_async_remote_copy(
            src_ref=x_source(side, event, j, from_input), dst_ref=relayed.at[event, n],
            send_sem=x_send.at[event % 2, side, j], recv_sem=r_recv.at[event, n],
            device_id={"cols": via[source]}, device_id_type=MESH)

    def second_hop(source, event, j):
        side, n, p = 2 - source, j - first_relayed(event), event % 2
        return pltpu.make_async_remote_copy(
            src_ref=relayed.at[event, n],
            dst_ref=field[p].at[1 + row(j), (1 - side) * (width + 1), inner],
            send_sem=f_send.at[event, n], recv_sem=x_recv.at[p, 1 - side, j],
            device_id={"cols": 3 - source}, device_id_type=MESH)

    def send_x(side, event, j, from_input=False):
        if not via:
            pl.when(has["cols", side])(lambda: x_face(side, event, j, from_input, side).start())
            return
        first = first_relayed(event)
        relay = jnp.logical_and(col == 2 - side, jnp.logical_and(j >= first, j < first + share))
        pl.when(relay)(lambda: first_hop(2 - side, event, j, from_input).start())
        pl.when(jnp.logical_and(has["cols", side], jnp.logical_not(relay)))(
            lambda: x_face(side, event, j, from_input, side).start())

    def send_both(event, j, from_input=False):
        if not via:
            for side in (0, 1):
                send_x(side, event, j, from_input)
            return
        pl.when(col == 1)(lambda: send_x(1, event, j, from_input))
        send_x(0, event, j, from_input)
        pl.when(col != 1)(lambda: send_x(1, event, j, from_input))

    def forward(event, j):
        for source in (1, 2):
            @pl.when(col == via[source])
            def _():
                n = j - first_relayed(event)
                pltpu.make_async_remote_copy(
                    src_ref=relayed.at[event, n], dst_ref=relayed.at[event, n],
                    send_sem=f_send.at[event, n], recv_sem=r_recv.at[event, n],
                    device_id={"cols": 3 - source}, device_id_type=MESH).wait_recv()
                second_hop(source, event, j).start()

    def by_side(axis, action):
        for side in (0, 1):
            pl.when(has[axis, side])(functools.partial(action, side))

    tracer_parts = [(0, EDGE + 1)]
    tracer_parts += [(EDGE + k * middle + 1, middle) for k in range(slots - 1)]
    tracer_parts += [(EDGE + (slots - 1) * middle + 1, middle - 2), (width - EDGE - 1, EDGE + 1)]

    def load_tracer(k):
        start, count = tracer_parts[k]
        return pltpu.make_async_copy(
            tracer.at[:, pl.ds(start, count)],
            field[0].at[pl.ds(1, rows), pl.ds(1 + start, count), inner], load_sem.at[0, k])

    def load_limit(k):
        start, count = span(k)
        return pltpu.make_async_copy(
            crowding.at[:, pl.ds(start, count)], limit.at[:, pl.ds(start, count)], load_sem.at[1, k])

    barrier = pltpu.get_barrier_semaphore()
    for axis in AXES:
        by_side(axis, lambda side: pl.semaphore_signal(
            barrier, inc=1, device_id=near[axis, side], device_id_type=MESH))
    if via:
        pl.semaphore_signal(barrier, inc=1, device_id={"cols": lax.rem(col + 2, 4)}, device_id_type=MESH)
    for k in (0, last, 1):
        load_tracer(k).start()
    for k in (1, 0, last):
        load_limit(k).start()
    for k in range(2, last):
        load_tracer(k).start()
        load_limit(k).start()
    pl.semaphore_wait(barrier, (1 if via else 0) + sum(jnp.where(has[key], 1, 0) for key in has))

    for j in range(rows):
        send_both(0, j, True)
    for k in [1, 0, last, *range(2, last)]:
        by_side("rows", lambda side: y_face(side, 0, k, True, side).start())
        if k in (0, last):
            for group in range(rows // half):
                by_side("slabs", lambda side: e_face(side, 0, k // last, group, True, side).start())
        else:
            by_side("slabs", lambda side: z_face(side, 0, k, True, side).start())

    def clear(axis, side):
        @pl.when(jnp.logical_not(has[axis, side]))
        def _():
            for p in (0, 1):
                if axis == "rows":
                    @pl.loop(1, width + 1)
                    def _(x):
                        field[p][side * (rows + 1), x, inner] = jnp.zeros((depth, species), jnp.float32)
                elif axis == "cols":
                    @pl.loop(1, rows + 1)
                    def _(y):
                        field[p][y, side * (width + 1), inner] = jnp.zeros((depth, species), jnp.float32)
                else:
                    @pl.loop(1, width + 1)
                    def _(x):
                        for y in range(1, rows + 1):
                            field[p][y, x, pl.ds(PAD - 1 + side * (depth + 1), 1)] = jnp.zeros((1, species), jnp.float32)

    for axis in AXES:
        for side in (0, 1):
            clear(axis, side)

    def advance(step, k):
        p = step % 2
        start, count = span(k)

        def store(x, y, at, value):
            if step == STEPS - 1:
                limit[y, start + x, pl.ds(at, 8)] = value
            else:
                field[1 - p][y + 1, 1 + start + x, pl.ds(PAD + at, 8)] = value

        stencil(step, field[p], limit, rows, depth, start, count, store)

    def advance_edges(step, y):
        p = step % 2
        tiles = depth // 8
        group = next(g for g in (4, 3, 2, 1) if tiles % g == 0)

        @pl.loop(0, tiles // group)
        def _(block):
            for n in range(group):
                at = pl.multiple_of(PAD + block * (8 * group) + 8 * n, 8)
                source = pl.multiple_of(block * (8 * group) + 8 * n, 8)
                for edge in (0, 1):
                    start = edge * (width - EDGE)

                    def cell(x, shift=0, up=0):
                        return field[p][1 + y + up, 1 + start + x, pl.ds(at + shift, 8)]

                    line = [cell(x) for x in range(-1, EDGE + 1)]
                    for x in range(EDGE):
                        here = line[x + 1]
                        around = (line[x] + line[x + 2]) + (cell(x, 0, -1) + cell(x, 0, 1))
                        around = around + (cell(x, -1) + cell(x, 1))
                        bound = limit[y, start + x, pl.ds(source, 8)]
                        if step == 0:
                            bound = bound + bound
                        value = scale(step) * (around + here * (6.0 - bound * here))
                        if step == STEPS - 1:
                            limit[y, start + x, pl.ds(source, 8)] = value
                        else:
                            field[1 - p][1 + y, 1 + start + x, pl.ds(at, 8)] = value

    def centre(step, k):
        p = step % 2
        if step == 0:
            load_limit(k).wait()
        by_side("rows", lambda side: y_face(1 - side, p, k, False, side).wait_recv())
        by_side("slabs", lambda side: z_face(1 - side, p, k, False, side).wait_recv())
        if step >= 1:
            by_side("rows", lambda side: y_face(side, 1 - p, k, False, side).wait_send())
            by_side("slabs", lambda side: z_face(side, 1 - p, k, False, side).wait_send())
        if step == STEPS - 1:
            pl.when(k <= slots - TAIL)(lambda: advance(step, k))
        else:
            advance(step, k)
        if step < STEPS - 1:
            by_side("rows", lambda side: y_face(side, 1 - p, k, False, side).start())
            by_side("slabs", lambda side: z_face(side, 1 - p, k, False, side).start())

    def edges(step, j):
        p = step % 2
        y = row(j)
        group = j // half

        def at_row(side):
            return jnp.logical_and(has["rows", side], y == side * (rows - 1))

        for side in (0, 1):
            @pl.when(at_row(side))
            def _():
                for k in (0, last):
                    y_face(1 - side, p, k, False, side).wait_recv()
                    if step >= 1:
                        y_face(side, 1 - p, k, False, side).wait_send()

        @pl.when(lax.rem(j, half) == 0)
        def _():
            for edge in (0, 1):
                by_side("slabs", lambda side: e_face(1 - side, p, edge, group, False, side).wait_recv())
                if step >= 1:
                    by_side("slabs", lambda side: e_face(side, 1 - p, edge, group, False, side).wait_send())

        by_side("cols", lambda side: x_face(1 - side, step, j, False, side).wait_recv())
        if step >= 1:
            by_side("cols", lambda side: x_face(side, step - 1, j, False, side).wait_send())
        advance_edges(step, y)
        if step < STEPS - 1:
            send_both(step + 1, j)
            for side in (0, 1):
                @pl.when(at_row(side))
                def _():
                    for k in (0, last):
                        y_face(side, 1 - p, k, False, side).start()

            @pl.when(lax.rem(j, half) == half - 1)
            def _():
                for edge in (0, 1):
                    by_side("slabs", lambda side: e_face(side, 1 - p, edge, group, False, side).start())

    forwards = {}
    if via:
        for event in range(STEPS):
            for n in range(share):
                j = first_relayed(event) + n
                when = (FIRST + n) if event == 0 else (event - 1) * slots + j + LATE
                forwards.setdefault(min(when, STEPS * slots - 1), []).append((event, j))

    for step in range(STEPS):
        if step == 0:
            for k in (0, last, 1):
                load_tracer(k).wait()

        @pl.loop(0, slots)
        def _(slot):
            if step > 0:
                centre(step, slot + 1)
            if step == 0:
                for k in range(2, last):
                    pl.when(slot == k - 1)(functools.partial(lambda k: load_tracer(k).wait(), k))
                centre(step, slot + 1)

                @pl.when(slot == 0)
                def _():
                    for k in (0, last):
                        load_limit(k).wait()
            for n in range(slots):
                for event, j in forwards.get(step * slots + n, []):
                    pl.when(slot == n)(functools.partial(forward, event, j))
            edges(step, slot)

    p = (STEPS - 1) % 2

    @pl.loop(1, last)
    def _(k):
        by_side("rows", lambda side: y_face(side, p, k, False, side).wait_send())
        by_side("slabs", lambda side: z_face(side, p, k, False, side).wait_send())

    for k in (0, last):
        by_side("rows", lambda side: y_face(side, p, k, False, side).wait_send())
        for group in range(rows // half):
            by_side("slabs", lambda side: e_face(side, p, k // last, group, False, side).wait_send())
    for j in range(rows):
        by_side("cols", lambda side: x_face(side, STEPS - 1, j, False, side).wait_send())
    for when in sorted(forwards):
        for event, j in forwards[when]:
            for source in (1, 2):
                pl.when(col == via[source])(lambda: second_hop(source, event, j).wait_send())


def relays(mesh):
    if mesh.shape["cols"] != 4:
        return None
    devices = mesh.devices.transpose([mesh.axis_names.index(axis) for axis in AXES])[0, :, 0]
    chips = [getattr(device, "coords", None) for device in devices]
    if any(chip is None for chip in chips):
        return None
    apart = sum(a != b for a, b in zip(chips[1], chips[2]))
    return VIA if apart > 1 else None


def solution(mesh):
    sizes = dict(mesh.shape)
    via = relays(mesh)

    def on_device(tracer, crowding):
        rows, width, depth, species = tracer.shape
        half = rows // 2 if rows % 2 == 0 else rows
        groups, share, parts = rows // half, max(1, rows // 2), rows + 2
        dma = pltpu.SemaphoreType.DMA
        padded = (rows + 2, width + 2, depth + 2 * PAD, species)
        vmem = pl.BlockSpec(memory_space=pltpu.VMEM)
        held = pl.pallas_call(
            functools.partial(kernel, sizes, via),
            out_shape=pltpu.VMEM((2 * rows + 2, *padded[1:]), jnp.float32),
            in_specs=[pl.BlockSpec(memory_space=pl.ANY)] * 2,
            out_specs=vmem,
            scratch_shapes=[
                pltpu.VMEM(padded, jnp.float32),
                dma((2, parts)),
                dma((2, 2, parts)), dma((2, 2, parts)),
                dma((2, 2, parts)), dma((2, 2, parts)),
                dma((2, 2, 2, groups)), dma((2, 2, 2, groups)),
                dma((2, 2, rows)), dma((2, 2, rows)),
                pltpu.VMEM((STEPS, share, depth, species), jnp.float32),
                dma((STEPS, share)), dma((STEPS, share)),
            ],
            compiler_params=pltpu.CompilerParams(
                collective_id=0, has_side_effects=True, vmem_limit_bytes=23 << 20),
        )(tracer, crowding)
        piece = next(n for n in (5, 6, 4, 3, 2, 1) if (width - 2 * EDGE) // rows % n == 0)
        return pl.pallas_call(
            write,
            out_shape=jax.ShapeDtypeStruct(tracer.shape, jnp.float32),
            in_specs=[vmem],
            out_specs=pl.BlockSpec(memory_space=pl.ANY),
            scratch_shapes=[pltpu.VMEM((RING, rows, piece, depth, species), jnp.float32),
                            dma((rows, 2)), dma((max(1, width // piece),))],
            compiler_params=pltpu.CompilerParams(vmem_limit_bytes=9 << 20),
        )(held)

    return jax.shard_map(
        on_device, mesh=mesh,
        in_specs=(P("rows", "cols", "slabs", None), P("rows", "cols", "slabs", None)),
        out_specs=P("rows", "cols", "slabs", None), check_vma=False)
```

```python
import functools

import jax
import jax.numpy as jnp
from jax import lax
from jax.experimental import pallas as pl
from jax.experimental.pallas import tpu as pltpu
from jax.sharding import PartitionSpec as P

STEPS = 4
EDGE = 2
VIA = {1: 3, 2: 0}
LATE = 1
FIRST = 0
PAD = 8
TAIL = 2
RING = 8
MESH = pl.DeviceIdType.MESH
AXES = ("rows", "cols", "slabs")


def scale(step):
    return 0.2 if step == 0 else 0.05 if step == STEPS - 1 else 0.1


def stencil(step, now, limit, rows, depth, start, count, store):
    @pl.loop(0, depth // 8)
    def _(tile):
        source = pl.multiple_of(tile * 8, 8)
        at = pl.multiple_of(PAD + tile * 8, 8)

        def cell(y, x, shift=0):
            return now[y, 1 + start + x, pl.ds(at + shift, 8)]

        here = [cell(y, 0) for y in range(rows + 2)]
        slant = [cell(y, -1) + here[y + 1] for y in range(1, rows + 1)]
        for x in range(count):
            after = [None, *[cell(y, x + 1) for y in range(1, rows + 1)], None]
            steep = [here[y] + after[y + 1] for y in range(rows)]
            for y in range(rows):
                middle = here[y + 1]
                around = (slant[y] + steep[y]) + (cell(y + 1, x, -1) + cell(y + 1, x, 1))
                bound = limit[y, start + x, pl.ds(source, 8)]
                if step == 0:
                    bound = bound + bound
                store(x, y, source, scale(step) * (around + middle * (6.0 - bound * middle)))
            if x < count - 1:
                after[0], after[-1] = cell(0, x + 1), cell(rows + 1, x + 1)
                slant = [*steep[1:], here[rows] + after[rows + 1]]
                here = after


def tail_start(rows, width):
    middle = (width - 2 * EDGE) // rows
    return EDGE + (rows - TAIL) * middle


def write(held, out, stage, store_sem, stage_sem):
    rows, width, depth, species = out.shape
    field = held.at[pl.ds(0, rows + 2)]
    limit = held.at[pl.ds(rows + 2, rows), pl.ds(0, width), pl.ds(0, depth)]
    first, end = tail_start(rows, width), width - EDGE
    ready = [pltpu.make_async_copy(
        limit.at[y, pl.ds(start, count)], out.at[y, pl.ds(start, count)], store_sem.at[y, n])
        for n, (start, count) in enumerate(((0, first), (end, EDGE))) for y in range(rows)]
    for copy in ready:
        copy.start()
    slots, _, piece = stage.shape[:3]
    copies = []
    for n in range((end - first) // piece):
        start, slot = first + n * piece, n % slots
        if n >= slots:
            copies[n - slots].wait()

        def store(x, y, at, value):
            stage[slot, y, x, pl.ds(at, 8)] = value

        stencil(STEPS - 1, field, limit, rows, depth, start, piece, store)
        copies.append(pltpu.make_async_copy(
            stage.at[slot], out.at[:, pl.ds(start, piece)], stage_sem.at[n]))
        copies[n].start()
    for copy in [*ready, *copies[max(0, len(copies) - slots):]]:
        copy.wait()


def kernel(sizes, via, tracer, crowding, held, even_field, load_sem,
           y_send, y_recv, z_send, z_recv, e_send, e_recv, x_send, x_recv,
           relayed, r_recv, f_send):
    rows, width, depth, species = tracer.shape
    slots = rows
    middle = (width - 2 * EDGE) // slots
    last = slots + 1
    half = rows // 2 if rows % 2 == 0 else rows
    share = rows // 2
    odd_field = held.at[pl.ds(0, rows + 2)]
    limit = held.at[pl.ds(rows + 2, rows), pl.ds(0, width), pl.ds(0, depth)]
    field = (even_field, odd_field)
    place = {axis: lax.axis_index(axis) for axis in AXES}
    has = {(axis, side): (place[axis] > 0) if side == 0 else (place[axis] < sizes[axis] - 1)
           for axis in AXES for side in (0, 1)}
    near = {(axis, side): {axis: jnp.clip(place[axis] + 2 * side - 1, 0, sizes[axis] - 1)}
            for axis in AXES for side in (0, 1)}
    col = place["cols"]
    upward = lax.rem(place["rows"], 2) == 1
    inner = pl.ds(PAD, depth)

    def row(j):
        return jnp.where(upward, j, rows - 1 - j)

    def span(k):
        if isinstance(k, int):
            if k == 0:
                return 0, EDGE
            if k == last:
                return width - EDGE, EDGE
        return EDGE + (k - 1) * middle, middle

    def remote(axis, to, src, dst, send, recv):
        return pltpu.make_async_remote_copy(
            src_ref=src, dst_ref=dst, send_sem=send, recv_sem=recv,
            device_id=near[axis, to], device_id_type=MESH)

    def y_face(side, p, k, from_input, to):
        start, count = span(k)
        cells, other = pl.ds(1 + start, count), 1 - side
        src = (tracer.at[side * (rows - 1), pl.ds(start, count)] if from_input
               else field[p].at[1 + side * (rows - 1), cells, inner])
        return remote("rows", to, src, field[p].at[other * (rows + 1), cells, inner],
                      y_send.at[p, side, k], y_recv.at[p, other, k])

    def z_face(side, p, k, from_input, to):
        start, count = span(k)
        cells, other, ys = pl.ds(1 + start, count), 1 - side, pl.ds(1, rows)
        src = (tracer.at[:, pl.ds(start, count), pl.ds(side * (depth - 1), 1)] if from_input
               else field[p].at[ys, cells, pl.ds(PAD + side * (depth - 1), 1)])
        return remote("slabs", to, src, field[p].at[ys, cells, pl.ds(PAD - 1 + other * (depth + 1), 1)],
                      z_send.at[p, side, k], z_recv.at[p, other, k])

    def e_face(side, p, edge, group, from_input, to):
        start, count = span(edge * last)
        cells, other = pl.ds(1 + start, count), 1 - side
        first = jnp.where(upward, group * half, rows - (group + 1) * half)
        src = (tracer.at[pl.ds(first, half), pl.ds(start, count), pl.ds(side * (depth - 1), 1)] if from_input
               else field[p].at[pl.ds(1 + first, half), cells, pl.ds(PAD + side * (depth - 1), 1)])
        dst = field[p].at[pl.ds(1 + first, half), cells, pl.ds(PAD - 1 + other * (depth + 1), 1)]
        return remote("slabs", to, src, dst, e_send.at[p, side, edge, group], e_recv.at[p, other, edge, group])

    def x_source(side, event, j, from_input):
        return (tracer.at[row(j), side * (width - 1)] if from_input
                else field[event % 2].at[1 + row(j), 1 + side * (width - 1), inner])

    def x_face(side, event, j, from_input, to):
        p, other = event % 2, 1 - side
        return remote("cols", to, x_source(side, event, j, from_input),
                      field[p].at[1 + row(j), other * (width + 1), inner],
                      x_send.at[p, side, j], x_recv.at[p, other, j])

    def first_relayed(event):
        return 0 if event % 2 == 1 else rows - share

    def first_hop(source, event, j, from_input):
        side, n = 2 - source, j - first_relayed(event)
        return pltpu.make_async_remote_copy(
            src_ref=x_source(side, event, j, from_input), dst_ref=relayed.at[event, n],
            send_sem=x_send.at[event % 2, side, j], recv_sem=r_recv.at[event, n],
            device_id={"cols": via[source]}, device_id_type=MESH)

    def second_hop(source, event, j):
        side, n, p = 2 - source, j - first_relayed(event), event % 2
        return pltpu.make_async_remote_copy(
            src_ref=relayed.at[event, n],
            dst_ref=field[p].at[1 + row(j), (1 - side) * (width + 1), inner],
            send_sem=f_send.at[event, n], recv_sem=x_recv.at[p, 1 - side, j],
            device_id={"cols": 3 - source}, device_id_type=MESH)

    def send_x(side, event, j, from_input=False):
        if not via:
            pl.when(has["cols", side])(lambda: x_face(side, event, j, from_input, side).start())
            return
        first = first_relayed(event)
        relay = jnp.logical_and(col == 2 - side, jnp.logical_and(j >= first, j < first + share))
        if not from_input:
            pl.when(relay)(lambda: first_hop(2 - side, event, j, from_input).start())
        pl.when(jnp.logical_and(has["cols", side], jnp.logical_not(relay)))(
            lambda: x_face(side, event, j, from_input, side).start())

    def send_both(event, j, from_input=False):
        if not via:
            for side in (0, 1):
                send_x(side, event, j, from_input)
            return
        pl.when(col == 1)(lambda: send_x(1, event, j, from_input))
        send_x(0, event, j, from_input)
        pl.when(col != 1)(lambda: send_x(1, event, j, from_input))

    def forward(event, j):
        for source in (1, 2):
            @pl.when(col == via[source])
            def _():
                n = j - first_relayed(event)
                pltpu.make_async_remote_copy(
                    src_ref=relayed.at[event, n], dst_ref=relayed.at[event, n],
                    send_sem=f_send.at[event, n], recv_sem=r_recv.at[event, n],
                    device_id={"cols": 3 - source}, device_id_type=MESH).wait_recv()
                second_hop(source, event, j).start()

    def by_side(axis, action):
        for side in (0, 1):
            pl.when(has[axis, side])(functools.partial(action, side))

    tracer_parts = [(0, EDGE + 1)]
    tracer_parts += [(EDGE + k * middle + 1, middle) for k in range(slots - 1)]
    tracer_parts += [(EDGE + (slots - 1) * middle + 1, middle - 2), (width - EDGE - 1, EDGE + 1)]

    def load_tracer(k):
        start, count = tracer_parts[k]
        return pltpu.make_async_copy(
            tracer.at[:, pl.ds(start, count)],
            field[0].at[pl.ds(1, rows), pl.ds(1 + start, count), inner], load_sem.at[0, k])

    def load_limit(k):
        start, count = span(k)
        return pltpu.make_async_copy(
            crowding.at[:, pl.ds(start, count)], limit.at[:, pl.ds(start, count)], load_sem.at[1, k])

    barrier = pltpu.get_barrier_semaphore()
    for axis in AXES:
        by_side(axis, lambda side: pl.semaphore_signal(
            barrier, inc=1, device_id=near[axis, side], device_id_type=MESH))
    if via:
        pl.semaphore_signal(barrier, inc=1, device_id={"cols": lax.rem(col + 2, 4)}, device_id_type=MESH)
    for k in (0, last, 1):
        load_tracer(k).start()
    for k in (1, 0, last):
        load_limit(k).start()
    for k in range(2, last):
        load_tracer(k).start()
        load_limit(k).start()
    pl.semaphore_wait(barrier, (1 if via else 0) + sum(jnp.where(has[key], 1, 0) for key in has))

    if via:
        for source in (1, 2):
            @pl.when(col == source)
            def _():
                for n in range(share):
                    first_hop(source, 0, first_relayed(0) + n, True).start()
    for j in range(rows):
        send_both(0, j, True)
    for k in [1, 0, last, *range(2, last)]:
        by_side("rows", lambda side: y_face(side, 0, k, True, side).start())
        if k in (0, last):
            for group in range(rows // half):
                by_side("slabs", lambda side: e_face(side, 0, k // last, group, True, side).start())
        else:
            by_side("slabs", lambda side: z_face(side, 0, k, True, side).start())

    def clear(axis, side):
        @pl.when(jnp.logical_not(has[axis, side]))
        def _():
            for p in (0, 1):
                if axis == "rows":
                    @pl.loop(1, width + 1)
                    def _(x):
                        field[p][side * (rows + 1), x, inner] = jnp.zeros((depth, species), jnp.float32)
                elif axis == "cols":
                    @pl.loop(1, rows + 1)
                    def _(y):
                        field[p][y, side * (width + 1), inner] = jnp.zeros((depth, species), jnp.float32)
                else:
                    @pl.loop(1, width + 1)
                    def _(x):
                        for y in range(1, rows + 1):
                            field[p][y, x, pl.ds(PAD - 1 + side * (depth + 1), 1)] = jnp.zeros((1, species), jnp.float32)

    for axis in AXES:
        for side in (0, 1):
            clear(axis, side)

    def advance(step, k):
        p = step % 2
        start, count = span(k)

        def store(x, y, at, value):
            if step == STEPS - 1:
                limit[y, start + x, pl.ds(at, 8)] = value
            else:
                field[1 - p][y + 1, 1 + start + x, pl.ds(PAD + at, 8)] = value

        stencil(step, field[p], limit, rows, depth, start, count, store)

    def advance_edges(step, y):
        p = step % 2
        tiles = depth // 8
        group = next(g for g in (4, 3, 2, 1) if tiles % g == 0)

        @pl.loop(0, tiles // group)
        def _(block):
            for n in range(group):
                at = pl.multiple_of(PAD + block * (8 * group) + 8 * n, 8)
                source = pl.multiple_of(block * (8 * group) + 8 * n, 8)
                for edge in (0, 1):
                    start = edge * (width - EDGE)

                    def cell(x, shift=0, up=0):
                        return field[p][1 + y + up, 1 + start + x, pl.ds(at + shift, 8)]

                    line = [cell(x) for x in range(-1, EDGE + 1)]
                    for x in range(EDGE):
                        here = line[x + 1]
                        around = (line[x] + line[x + 2]) + (cell(x, 0, -1) + cell(x, 0, 1))
                        around = around + (cell(x, -1) + cell(x, 1))
                        bound = limit[y, start + x, pl.ds(source, 8)]
                        if step == 0:
                            bound = bound + bound
                        value = scale(step) * (around + here * (6.0 - bound * here))
                        if step == STEPS - 1:
                            limit[y, start + x, pl.ds(source, 8)] = value
                        else:
                            field[1 - p][1 + y, 1 + start + x, pl.ds(at, 8)] = value

    def centre(step, k):
        p = step % 2
        if step == 0:
            load_limit(k).wait()
        by_side("rows", lambda side: y_face(1 - side, p, k, False, side).wait_recv())
        by_side("slabs", lambda side: z_face(1 - side, p, k, False, side).wait_recv())
        if step >= 1:
            by_side("rows", lambda side: y_face(side, 1 - p, k, False, side).wait_send())
            by_side("slabs", lambda side: z_face(side, 1 - p, k, False, side).wait_send())
        if step == STEPS - 1:
            pl.when(k <= slots - TAIL)(lambda: advance(step, k))
        else:
            advance(step, k)
        if step < STEPS - 1:
            by_side("rows", lambda side: y_face(side, 1 - p, k, False, side).start())
            by_side("slabs", lambda side: z_face(side, 1 - p, k, False, side).start())

    def edges(step, j):
        p = step % 2
        y = row(j)
        group = j // half

        def at_row(side):
            return jnp.logical_and(has["rows", side], y == side * (rows - 1))

        for side in (0, 1):
            @pl.when(at_row(side))
            def _():
                for k in (0, last):
                    y_face(1 - side, p, k, False, side).wait_recv()
                    if step >= 1:
                        y_face(side, 1 - p, k, False, side).wait_send()

        @pl.when(lax.rem(j, half) == 0)
        def _():
            for edge in (0, 1):
                by_side("slabs", lambda side: e_face(1 - side, p, edge, group, False, side).wait_recv())
                if step >= 1:
                    by_side("slabs", lambda side: e_face(side, 1 - p, edge, group, False, side).wait_send())

        by_side("cols", lambda side: x_face(1 - side, step, j, False, side).wait_recv())
        if step >= 1:
            by_side("cols", lambda side: x_face(side, step - 1, j, False, side).wait_send())
        advance_edges(step, y)
        if step < STEPS - 1:
            send_both(step + 1, j)
            for side in (0, 1):
                @pl.when(at_row(side))
                def _():
                    for k in (0, last):
                        y_face(side, 1 - p, k, False, side).start()

            @pl.when(lax.rem(j, half) == half - 1)
            def _():
                for edge in (0, 1):
                    by_side("slabs", lambda side: e_face(side, 1 - p, edge, group, False, side).start())

    forwards = {}
    if via:
        for event in range(STEPS):
            for n in range(share):
                j = first_relayed(event) + n
                when = (FIRST + n) if event == 0 else (event - 1) * slots + j + LATE
                forwards.setdefault(min(when, STEPS * slots - 1), []).append((event, j))

    for step in range(STEPS):
        if step == 0:
            for k in (0, last, 1):
                load_tracer(k).wait()

        @pl.loop(0, slots)
        def _(slot):
            if step > 0:
                centre(step, slot + 1)
            if step == 0:
                for k in range(2, last):
                    pl.when(slot == k - 1)(functools.partial(lambda k: load_tracer(k).wait(), k))
                centre(step, slot + 1)

                @pl.when(slot == 0)
                def _():
                    for k in (0, last):
                        load_limit(k).wait()
            for n in range(slots):
                for event, j in forwards.get(step * slots + n, []):
                    pl.when(slot == n)(functools.partial(forward, event, j))
            edges(step, slot)

    p = (STEPS - 1) % 2

    @pl.loop(1, last)
    def _(k):
        by_side("rows", lambda side: y_face(side, p, k, False, side).wait_send())
        by_side("slabs", lambda side: z_face(side, p, k, False, side).wait_send())

    for k in (0, last):
        by_side("rows", lambda side: y_face(side, p, k, False, side).wait_send())
        for group in range(rows // half):
            by_side("slabs", lambda side: e_face(side, p, k // last, group, False, side).wait_send())
    for j in range(rows):
        by_side("cols", lambda side: x_face(side, STEPS - 1, j, False, side).wait_send())
    for when in sorted(forwards):
        for event, j in forwards[when]:
            for source in (1, 2):
                pl.when(col == via[source])(lambda: second_hop(source, event, j).wait_send())


def relays(mesh):
    if mesh.shape["cols"] != 4:
        return None
    devices = mesh.devices.transpose([mesh.axis_names.index(axis) for axis in AXES])[0, :, 0]
    chips = [getattr(device, "coords", None) for device in devices]
    if any(chip is None for chip in chips):
        return None
    apart = sum(a != b for a, b in zip(chips[1], chips[2]))
    return VIA if apart > 1 else None


def solution(mesh):
    sizes = dict(mesh.shape)
    via = relays(mesh)

    def on_device(tracer, crowding):
        rows, width, depth, species = tracer.shape
        half = rows // 2 if rows % 2 == 0 else rows
        groups, share, parts = rows // half, max(1, rows // 2), rows + 2
        dma = pltpu.SemaphoreType.DMA
        padded = (rows + 2, width + 2, depth + 2 * PAD, species)
        vmem = pl.BlockSpec(memory_space=pltpu.VMEM)
        held = pl.pallas_call(
            functools.partial(kernel, sizes, via),
            out_shape=pltpu.VMEM((2 * rows + 2, *padded[1:]), jnp.float32),
            in_specs=[pl.BlockSpec(memory_space=pl.ANY)] * 2,
            out_specs=vmem,
            scratch_shapes=[
                pltpu.VMEM(padded, jnp.float32),
                dma((2, parts)),
                dma((2, 2, parts)), dma((2, 2, parts)),
                dma((2, 2, parts)), dma((2, 2, parts)),
                dma((2, 2, 2, groups)), dma((2, 2, 2, groups)),
                dma((2, 2, rows)), dma((2, 2, rows)),
                pltpu.VMEM((STEPS, share, depth, species), jnp.float32),
                dma((STEPS, share)), dma((STEPS, share)),
            ],
            compiler_params=pltpu.CompilerParams(
                collective_id=0, has_side_effects=True, vmem_limit_bytes=23 << 20),
        )(tracer, crowding)
        piece = next(n for n in (5, 6, 4, 3, 2, 1) if (width - 2 * EDGE) // rows % n == 0)
        return pl.pallas_call(
            write,
            out_shape=jax.ShapeDtypeStruct(tracer.shape, jnp.float32),
            in_specs=[vmem],
            out_specs=pl.BlockSpec(memory_space=pl.ANY),
            scratch_shapes=[pltpu.VMEM((RING, rows, piece, depth, species), jnp.float32),
                            dma((rows, 2)), dma((max(1, width // piece),))],
            compiler_params=pltpu.CompilerParams(vmem_limit_bytes=9 << 20),
        )(held)

    return jax.shard_map(
        on_device, mesh=mesh,
        in_specs=(P("rows", "cols", "slabs", None), P("rows", "cols", "slabs", None)),
        out_specs=P("rows", "cols", "slabs", None), check_vma=False)
```
